256 devices in a mesh: group: 8 (over x, core), member: 32 (over z, y).
Axes of the slice: x: 4, y: 4, z: 8, core: 2. Of those that a mesh axis runs over, the one named last changes fastest.
Arguments:
- queries: bfloat16 [256, 32, 128], P(('group', 'member')), may hold values from -1.2 to 1.2
- pages: bfloat16 [1536, 1024, 128], P(('group', 'member')), may hold values from -1.2 to 1.2
- users: int32 [1536, 32], P(('group', 'member')), may hold values from 0 to 255, as said below
- page_count: int32 [1536], P(('group', 'member')), may hold values from 1 to 32
- teacher: float32 [1536, 32], P(('group', 'member')), may hold values from 4 to 12
Outputs:
- scores: float32 [1536, 32], P(('group', 'member'))
- query_grad: float32 [256, 32, 128], P(('group', 'member'))
- page_grad: bfloat16 [1536, 1024, 128], P(('group', 'member'))
The draws below stay inside these ranges and needn't reach their ends.
Inputs may be any that keep to these rules, and one draw needn't show every extreme that they name: `users`: slots at or past page_count hold valid ids that are ignored. Queries are numbered in the order of their owning devices. Over the slots of the pages of one device, exactly 8 distinct queries of each group (of 32 consecutive query ids) appear, counting dead slots too.
All inputs are finite; a program needn't handle non-finite values.
Results may differ from the reference program's by a relative error of at most 0.014.
Values may be sent and summed in bfloat16 or wider, within the bound.
A program may use at most 64 MiB of HBM per device.

```python
import jax
import jax.numpy as jnp
from jax import lax

DIM = 128
QTOK = 32
PTOK = 1024
USE = 32
CAP = 8
Q_DEV = 1
PG_DEV = 6
QUERIES = 256
PAGES = 1536
N_GROUP = 8
N_MEMBER = 32
DEVICES = 256


def draw_pages(key, part):
    noise_key = jax.random.fold_in(key, 11)
    values = jnp.clip(0.1 * jax.random.normal(noise_key, (PAGES, PTOK, DIM), jnp.float32), -0.6, 0.6)
    return values.astype(jnp.bfloat16)


def draw_queries(key, part):
    noise_key = jax.random.fold_in(key, 13)
    values = jnp.clip(0.1 * jax.random.normal(noise_key, (QUERIES, QTOK, DIM), jnp.float32), -0.6, 0.6)
    return values.astype(jnp.bfloat16)


def member_picks(member_key):
    return jax.random.permutation(member_key, N_MEMBER * Q_DEV)[:CAP]


def device_order(device_key):
    return jax.random.permutation(device_key, N_GROUP * CAP)


def slot_order(device_key):
    return jax.random.permutation(device_key, PG_DEV * USE)


def draw_users(key, part):
    group_rows = N_MEMBER * Q_DEV
    slot_total = PG_DEV * USE
    listed = N_GROUP * CAP
    pick_keys = jax.random.split(jax.random.fold_in(key, 21), DEVICES * N_GROUP)
    picks = jax.vmap(member_picks)(pick_keys).astype(jnp.int32).reshape(DEVICES, N_GROUP, CAP)
    offsets = (jnp.arange(N_GROUP, dtype=jnp.int32) * group_rows)[None, :, None]
    candidates = (picks + offsets).reshape(DEVICES, listed)
    first = jax.vmap(device_order)(jax.random.split(jax.random.fold_in(key, 22), DEVICES)).astype(jnp.int32)
    extra_one = jax.random.randint(jax.random.fold_in(key, 23), (DEVICES, slot_total - listed), 0, listed)
    extra_two = jax.random.randint(jax.random.fold_in(key, 24), (DEVICES, slot_total - listed), 0, listed)
    extra = jnp.minimum(extra_one, extra_two).astype(jnp.int32)
    chosen = jnp.concatenate([first, extra], axis=1)
    order = jax.vmap(slot_order)(jax.random.split(jax.random.fold_in(key, 25), DEVICES)).astype(jnp.int32)
    chosen = jnp.take_along_axis(chosen, order, axis=1)
    result = jnp.take_along_axis(candidates, chosen, axis=1)
    return result.reshape(PAGES, USE).astype(jnp.int32)


def touch_ends(drawn, rng, smallest, largest):
    longest = drawn.shape.index(max(drawn.shape))
    spots = []
    for shift in (0, 1):
        where = [jax.random.randint(jax.random.fold_in(rng, axis), (), 0, length) for axis, length in enumerate(drawn.shape)]
        where[longest] = (where[longest] + shift) % drawn.shape[longest]
        spots.append(tuple(where))
    return drawn.at[spots[0]].set(smallest).at[spots[1]].set(largest)


def shard_levels(stream_key, shape, cuts, least, high):
    loudness, own = 1.0, jax.random.fold_in(stream_key, 6)
    for position, blocks in cuts:
        heights = jnp.exp(jax.random.uniform(jax.random.fold_in(own, position), (blocks,), jnp.float32, least / len(cuts), high / len(cuts)))
        loudness = loudness * jnp.repeat(heights, shape[position] // blocks).reshape([-1 if axis == position else 1 for axis in range(len(shape))])
    return loudness


def setup_inputs(seed: int = 0) -> dict:
    key_list = jax.random.split(jax.random.key(seed), 6)
    return {
        "queries": draw_queries(jax.random.fold_in(key_list[5], 71), 0),
        "pages": draw_pages(jax.random.fold_in(key_list[5], 71), 0),
        "users": draw_users(jax.random.fold_in(key_list[5], 71), 0),
        "page_count": touch_ends(jax.random.randint(key_list[3], (PAGES,), 1, USE + 1), jax.random.fold_in(key_list[3], 1), 1, USE).astype(jnp.int32),
        "teacher": jnp.clip(4.0 + 8.0 * jax.random.uniform(key_list[4], (PAGES, USE), jnp.float32) ** shard_levels(key_list[4], (PAGES, USE), ((0, 256),), -0.2, 0.2), 4.0, 12.0),
    }


normalized_exponent_divisor = 0.05


def reference(queries, pages, users, page_count, teacher):
    query_f32 = queries.astype(jnp.float32)
    slot_ids = jnp.arange(USE).astype(jnp.int32)

    def page_step(grad_total, inputs):
        page_tile, user_row, active_total, teacher_row = inputs
        document_single_float = page_tile.astype(jnp.float32)
        chosen = query_f32[user_row]
        cosine_affinity = jnp.einsum("uqd,pd->uqp", chosen, document_single_float)
        pairing_coefficients = jax.nn.softmax(cosine_affinity / normalized_exponent_divisor, axis=-1)
        aligned_rating = jnp.sum(pairing_coefficients * cosine_affinity, axis=-1)
        score = jnp.sum(aligned_rating, axis=-1)
        live = slot_ids < active_total
        unaligned_rating = jnp.where(live, score - teacher_row, jnp.zeros_like(score))
        rating_gradient_factor = unaligned_rating[:, None, None] * pairing_coefficients * (1.0 + (cosine_affinity - aligned_rating[:, :, None]) / normalized_exponent_divisor)
        rating_gradient_factor = lax.optimization_barrier(rating_gradient_factor.astype(jnp.bfloat16)).astype(jnp.float32)
        query_part = jnp.einsum("uqp,pd->uqd", rating_gradient_factor, document_single_float)
        page_part = jnp.einsum("uqp,uqd->pd", rating_gradient_factor, chosen)
        grad_total = grad_total.at[user_row].add(query_part)
        return grad_total, (jnp.where(live, score, jnp.zeros_like(score)), page_part.astype(jnp.bfloat16))

    initial = jnp.zeros(queries.shape, jnp.float32)
    query_grad, (scores, page_grad) = lax.scan(page_step, initial, (pages, users, page_count, teacher))
    return scores, query_grad, page_grad
```

```python
import functools
import math

import jax
import jax.numpy as jnp
from jax import lax
from jax.experimental import pallas as pl
from jax.experimental.pallas import tpu as pltpu
from jax.sharding import PartitionSpec as P

MESH = pl.DeviceIdType.MESH
CAP = 8
GROUPS = 8
MEMBERS = 32
TOK = 32
DIM = 128
CHUNK = 8
LANES = CHUNK * TOK
INV_AT = 32
SCALE = math.log2(math.e) / 0.05
LN2 = math.log(2.0)


def greet(me_g, me_m):
    barrier = pltpu.get_barrier_semaphore()

    def to_member(k, carry):
        pl.semaphore_signal(
            barrier, inc=1, device_id=(me_g, (me_m + k) % MEMBERS), device_id_type=MESH
        )
        return carry

    lax.fori_loop(1, MEMBERS, to_member, 0)
    for k in range(1, GROUPS):
        pl.semaphore_signal(
            barrier, inc=1, device_id=((me_g + k) % GROUPS, me_m), device_id_type=MESH
        )
    return barrier


def fetch_kernel(
    query_ref, users_ref, picked_ref, lut_ref, info_ref,
    table, asks_out, asks_in, asks_smem, chosen,
    q_send, q_recv, a_send, a_recv, c_send, c_recv, local_sem,
):
    me_g = lax.axis_index("group")
    me_m = lax.axis_index("member")
    barrier = greet(me_g, me_m)

    total = GROUPS * MEMBERS
    rows = users_ref.shape[0]
    qid = lax.broadcasted_iota(jnp.int32, (total, users_ref.shape[1]), 0)
    hit = jnp.zeros(qid.shape, jnp.float32)
    for p in range(rows):
        hit = jnp.where(users_ref[p : p + 1, :] == qid, 1.0, hit)
    count = lax.dot_general(
        jnp.ones((8, users_ref.shape[1]), jnp.bfloat16),
        hit.astype(jnp.bfloat16),
        (((1,), (1,)), ((), ())),
        preferred_element_type=jnp.float32,
    )
    used = jnp.where(count > 0.5, 1.0, 0.0)
    ri = lax.broadcasted_iota(jnp.int32, (total, total), 0)
    ci = lax.broadcasted_iota(jnp.int32, (total, total), 1)
    before = jnp.where((ri < ci) & ((ri >> 5) == (ci >> 5)), 1.0, 0.0).astype(jnp.bfloat16)
    rank = jnp.dot(used.astype(jnp.bfloat16), before, preferred_element_type=jnp.float32)
    lane8 = lax.broadcasted_iota(jnp.int32, (8, total), 1)
    sub8 = lax.broadcasted_iota(jnp.int32, (8, total), 0)
    lut_ref[...] = (lane8 >> 5) * CAP + rank.astype(jnp.int32)
    of_group = (lane8 >> 5) == sub8
    k_id = lax.broadcasted_iota(jnp.int32, (128, total), 0).astype(jnp.float32)
    local_id = (lax.broadcasted_iota(jnp.int32, (128, total), 1) & 31).astype(jnp.float32)
    named = jnp.where((k_id == rank[0:1]) & (used[0:1] > 0.5), local_id, 0.0)
    ids = lax.dot_general(
        jnp.where(of_group, 1.0, 0.0).astype(jnp.bfloat16),
        named.astype(jnp.bfloat16),
        (((1,), (1,)), ((), ())),
        preferred_element_type=jnp.float32,
    )
    inverse = jnp.where(of_group, jnp.where(used > 0.5, rank, float(CAP)), 0.0)
    fold_r = lax.broadcasted_iota(jnp.int32, (total, 128), 0)
    fold_c = lax.broadcasted_iota(jnp.int32, (total, 128), 1)
    fold = jnp.where(fold_c == INV_AT + (fold_r & 31), 1.0, 0.0).astype(jnp.bfloat16)
    spread = jnp.dot(inverse.astype(jnp.bfloat16), fold, preferred_element_type=jnp.float32)
    asks = (ids + spread).astype(jnp.int32)
    for g in range(GROUPS):
        asks_out[g] = asks[g : g + 1, :]

    pl.semaphore_wait(barrier, MEMBERS - 1 + GROUPS - 1)

    def query_copy(k, src_m):
        peer = (me_m + k) % MEMBERS
        return pltpu.make_async_remote_copy(
            src_ref=query_ref.at[0],
            dst_ref=table.at[src_m],
            send_sem=q_send.at[k],
            recv_sem=q_recv.at[src_m],
            device_id=(me_g, peer),
            device_id_type=MESH,
        )

    def ask_copy(k, src_g):
        peer = (me_g + k) % GROUPS
        return pltpu.make_async_remote_copy(
            src_ref=asks_out.at[peer],
            dst_ref=asks_in.at[src_g],
            send_sem=a_send.at[k],
            recv_sem=a_recv.at[src_g],
            device_id=(peer, me_m),
            device_id_type=MESH,
        )

    def chosen_copy(k, src_g):
        peer = (me_g + k) % GROUPS
        return pltpu.make_async_remote_copy(
            src_ref=chosen.at[k],
            dst_ref=picked_ref.at[pl.ds(src_g * CAP, CAP)],
            send_sem=c_send.at[k],
            recv_sem=c_recv.at[src_g],
            device_id=(peer, me_m),
            device_id_type=MESH,
        )

    for k in range(1, GROUPS):
        ask_copy(k, me_g).start()

    def send_query(k, carry):
        query_copy(k, me_m).start()
        return carry

    lax.fori_loop(1, MEMBERS, send_query, 0)
    table[me_m] = query_ref[0]
    asks_in[me_g] = asks_out[me_g]
    for k in range(1, GROUPS):
        ask_copy(k, (me_g + k) % GROUPS).wait_recv()
    to_smem = pltpu.make_async_copy(asks_in, asks_smem, local_sem)
    to_smem.start()
    info_ref[...] = asks_in[...]
    to_smem.wait()

    def got_query(k, carry):
        query_copy(k, (me_m + k) % MEMBERS).wait_recv()
        return carry

    lax.fori_loop(1, MEMBERS, got_query, 0)
    for k in (4, 5, 2, 3, 6, 7, 1):
        peer = (me_g + k) % GROUPS
        for n in range(CAP):
            chosen[k, n] = table[asks_smem[peer, 0, n] & (MEMBERS - 1)]
        chosen_copy(k, me_g).start()
    for n in range(CAP):
        picked_ref[me_g * CAP + n] = table[asks_smem[me_g, 0, n] & (MEMBERS - 1)]
    for k in range(1, GROUPS):
        chosen_copy(k, (me_g + k) % GROUPS).wait_recv()
    for k in range(1, GROUPS):
        ask_copy(k, me_g).wait_send()
        chosen_copy(k, me_g).wait_send()

    def sent_query(k, carry):
        query_copy(k, me_m).wait_send()
        return carry

    lax.fori_loop(1, MEMBERS, sent_query, 0)


def fetch(queries, users):
    return pl.pallas_call(
        fetch_kernel,
        out_shape=(
            jax.ShapeDtypeStruct((GROUPS * CAP, TOK, DIM), jnp.bfloat16),
            jax.ShapeDtypeStruct((8, GROUPS * MEMBERS), jnp.int32),
            jax.ShapeDtypeStruct((GROUPS, 1, 128), jnp.int32),
        ),
        in_specs=[pl.BlockSpec(memory_space=pltpu.VMEM)] * 2,
        out_specs=[pl.BlockSpec(memory_space=pltpu.VMEM)] * 3,
        scratch_shapes=[
            pltpu.VMEM((MEMBERS, TOK, DIM), jnp.bfloat16),
            pltpu.VMEM((GROUPS, 1, 128), jnp.int32),
            pltpu.VMEM((GROUPS, 1, 128), jnp.int32),
            pltpu.SMEM((GROUPS, 1, 128), jnp.int32),
            pltpu.VMEM((GROUPS, CAP, TOK, DIM), jnp.bfloat16),
            pltpu.SemaphoreType.DMA((MEMBERS,)),
            pltpu.SemaphoreType.DMA((MEMBERS,)),
            pltpu.SemaphoreType.DMA((GROUPS,)),
            pltpu.SemaphoreType.DMA((GROUPS,)),
            pltpu.SemaphoreType.DMA((GROUPS,)),
            pltpu.SemaphoreType.DMA((GROUPS,)),
            pltpu.SemaphoreType.DMA,
        ],
        compiler_params=pltpu.CompilerParams(collective_id=0, has_side_effects=True),
        name="fetch",
    )(queries, users)


def split_dot(value, ones):
    high = value.astype(jnp.bfloat16)
    rest = value - high.astype(jnp.float32)
    mid = rest.astype(jnp.bfloat16)
    low = (rest - mid.astype(jnp.float32)).astype(jnp.bfloat16)
    dot = functools.partial(jnp.dot, preferred_element_type=jnp.float32)
    return dot(high, ones) + (dot(mid, ones) + dot(low, ones))


def match_kernel(
    users_ref, lut_ref, count_ref, teacher_ref, picked_ref, pages_ref,
    scores_ref, rows_ref, grad_ref,
    chunks, page_t, sims, logit, expo, stats, acc, row_acc, score_l, same_slot,
):
    n_pages, n_tok, _ = pages_ref.shape
    per_page = users_ref.shape[1] // CHUNK
    blocks = n_tok // 256

    def list_chunk(n, total):
        p = n // per_page
        alive = (n % per_page) * CHUNK < count_ref[p]

        @pl.when(alive)
        def _():
            chunks[total] = n

        return total + alive.astype(jnp.int32)

    total = lax.fori_loop(0, n_pages * per_page, list_chunk, 0)
    chunks[total] = chunks[total - 1]
    for p in range(n_pages):
        page_t[p] = pages_ref[p].T
    acc[...] = jnp.zeros_like(acc)
    row_acc[...] = jnp.zeros_like(row_acc)
    score_l[...] = jnp.zeros_like(score_l)
    seg_r = lax.broadcasted_iota(jnp.int32, (LANES, LANES), 0) >> 5
    seg_c = lax.broadcasted_iota(jnp.int32, (LANES, LANES), 1) >> 5
    same_slot[...] = jnp.where(seg_r == seg_c, 1.0, 0.0).astype(jnp.bfloat16)
    slot_of_lane = lax.broadcasted_iota(jnp.int32, (8, LANES), 1) >> 5

    def where_of(n):
        code = chunks[n]
        return code // per_page, code % per_page

    def picked_at(p, c, k):
        return lut_ref[0, users_ref[p, c * CHUNK + k]]

    def chosen_of(p, c):
        return jnp.concatenate(
            [picked_ref[picked_at(p, c, k)] for k in range(CHUNK)], axis=0
        )

    def fold8(value, op):
        parts = [value[8 * i : 8 * i + 8] for i in range(value.shape[0] // 8)]
        while len(parts) > 1:
            parts = [
                op(parts[i], parts[i + 1]) if i + 1 < len(parts) else parts[i]
                for i in range(0, len(parts), 2)
            ]
        return parts[0]

    def similar_of(n):
        p, c = where_of(n)
        chosen = chosen_of(p, c)
        top = None
        for b in range(blocks):
            block = lax.dot_general(
                pages_ref[p, 256 * b : 256 * b + 256, :],
                chosen,
                (((1,), (1,)), ((), ())),
                preferred_element_type=jnp.float32,
            )
            sims[256 * b : 256 * b + 256, :] = block
            high = fold8(block, jnp.maximum)
            top = high if top is None else jnp.maximum(top, high)
        return jnp.broadcast_to(jnp.max(top, axis=0, keepdims=True), (8, LANES))

    def weigh(top):
        mass = jnp.zeros((8, LANES), jnp.float32)
        moment = jnp.zeros((8, LANES), jnp.float32)
        top64 = jnp.concatenate([top] * 8, axis=0)
        for b in range(n_tok // 64):
            at = slice(64 * b, 64 * b + 64)
            t = (sims[at, :] - top64) * SCALE
            e = jnp.exp2(t)
            mass += fold8(e, jnp.add)
            moment += fold8(e * t, jnp.add)
            logit[at, :] = t
            expo[at, :] = e
        return mass, moment

    def finish(n, top, mass, moment):
        p, c = where_of(n)
        mass = jnp.broadcast_to(jnp.sum(mass, axis=0, keepdims=True), (8, LANES))
        moment = jnp.broadcast_to(jnp.sum(moment, axis=0, keepdims=True), (8, LANES))
        mean = moment / mass
        matched = top + mean * (1.0 / SCALE)
        score = split_dot(matched, same_slot[...])
        taught = jnp.zeros((8, LANES), jnp.float32)
        for k in range(CHUNK):
            taught = jnp.where(slot_of_lane == k, teacher_ref[p, c * CHUNK + k], taught)
        live = slot_of_lane + c * CHUNK < count_ref[p]
        score_l[c, pl.ds(p, 1), :] = jnp.where(live, score, 0.0)[0:1]
        part = jnp.where(live, score - taught, 0.0) / mass
        slant = part * LN2
        base = part - slant * mean
        chosen = chosen_of(p, c)
        base64 = jnp.concatenate([base] * 8, axis=0)
        slant64 = jnp.concatenate([slant] * 8, axis=0)
        query_t = jnp.zeros((DIM, LANES), jnp.float32)
        for b in range(blocks):
            parts = []
            for i in range(4):
                at = slice(256 * b + 64 * i, 256 * b + 64 * i + 64)
                parts.append(
                    (expo[at, :] * (base64 + slant64 * logit[at, :])).astype(jnp.bfloat16)
                )
            slope = jnp.concatenate(parts, axis=0)
            at = slice(256 * b, 256 * b + 256)
            acc[p, at, :] += jnp.dot(slope, chosen, preferred_element_type=jnp.float32)
            query_t += jnp.dot(page_t[p, :, at], slope, preferred_element_type=jnp.float32)
        query_part = query_t.T
        for k in range(CHUNK):
            row_acc[picked_at(p, c, k)] += query_part[TOK * k : TOK * k + TOK]

    def step(n, carry):
        top = similar_of(n)
        mass, moment = weigh(top)
        finish(n, top, mass, moment)
        return carry

    lax.fori_loop(0, total, step, 0)

    col = lax.broadcasted_iota(jnp.int32, (LANES, 128), 1)
    row = lax.broadcasted_iota(jnp.int32, (LANES, 128), 0)
    out = jnp.zeros((8, 128), jnp.float32)
    for c in range(per_page):
        take = jnp.where(row == (col - c * CHUNK) * TOK, 1.0, 0.0)
        out += split_dot(score_l[c], take.astype(jnp.bfloat16))
    scores_ref[...] = out[: scores_ref.shape[0], : scores_ref.shape[1]]
    for p in range(n_pages):
        grad_ref[p] = acc[p].astype(jnp.bfloat16)
    rows_ref[...] = row_acc[...].astype(jnp.bfloat16)


def match(users, lut, page_count, teacher, picked, pages):
    n_pages, n_tok, _ = pages.shape
    per_page = users.shape[1] // CHUNK
    smem = pl.BlockSpec(memory_space=pltpu.SMEM)
    vmem = pl.BlockSpec(memory_space=pltpu.VMEM)
    return pl.pallas_call(
        match_kernel,
        out_shape=(
            jax.ShapeDtypeStruct(users.shape, jnp.float32),
            jax.ShapeDtypeStruct(picked.shape, jnp.bfloat16),
            jax.ShapeDtypeStruct(pages.shape, jnp.bfloat16),
        ),
        in_specs=[smem, smem, smem, smem, vmem, vmem],
        out_specs=[vmem, vmem, vmem],
        scratch_shapes=[
            pltpu.SMEM((n_pages * per_page + 1,), jnp.int32),
            pltpu.VMEM((n_pages, DIM, n_tok), jnp.bfloat16),
            pltpu.VMEM((n_tok, LANES), jnp.float32),
            pltpu.VMEM((n_tok, LANES), jnp.float32),
            pltpu.VMEM((n_tok, LANES), jnp.float32),
            pltpu.VMEM((8, LANES), jnp.float32),
            pltpu.VMEM((n_pages, n_tok, DIM), jnp.float32),
            pltpu.VMEM(picked.shape, jnp.float32),
            pltpu.VMEM((per_page, 8, LANES), jnp.float32),
            pltpu.VMEM((LANES, LANES), jnp.bfloat16),
        ],
        compiler_params=pltpu.CompilerParams(vmem_limit_bytes=40 << 20),
        name="match",
    )(users, lut, page_count, teacher, picked, pages)


def give_kernel(
    rows_ref, info_ref, out_ref,
    landed, table, parts, r_send, r_recv, t_send, t_recv,
):
    me_g = lax.axis_index("group")
    me_m = lax.axis_index("member")
    barrier = greet(me_g, me_m)
    for s in range(GROUPS):
        for spare in range(CAP, 2 * CAP):
            landed[s, spare] = jnp.zeros((TOK, DIM), jnp.bfloat16)
    pl.semaphore_wait(barrier, MEMBERS - 1 + GROUPS - 1)

    def row_copy(k, src_g):
        peer = (me_g + k) % GROUPS
        return pltpu.make_async_remote_copy(
            src_ref=rows_ref.at[pl.ds(peer * CAP, CAP)],
            dst_ref=landed.at[src_g, pl.ds(0, CAP)],
            send_sem=r_send.at[k],
            recv_sem=r_recv.at[src_g],
            device_id=(peer, me_m),
            device_id_type=MESH,
        )

    def table_copy(k, src_m):
        peer = (me_m + k) % MEMBERS
        return pltpu.make_async_remote_copy(
            src_ref=table.at[k],
            dst_ref=parts.at[src_m],
            send_sem=t_send.at[k],
            recv_sem=t_recv.at[src_m],
            device_id=(me_g, peer),
            device_id_type=MESH,
        )

    for k in (4, 5, 2, 3, 6, 7, 1):
        row_copy(k, me_g).start()
    for n in range(CAP):
        landed[me_g, n] = rows_ref[me_g * CAP + n]
    for k in range(1, GROUPS):
        row_copy(k, (me_g + k) % GROUPS).wait_recv()

    def total_of(owner):
        total = jnp.zeros((TOK, DIM), jnp.float32)
        for s in range(GROUPS):
            total += landed[s, info_ref[s, 0, INV_AT + owner] & (2 * CAP - 1)].astype(jnp.float32)
        return total.astype(jnp.bfloat16)

    def send_table(n, carry):
        k = jnp.where(n >= MEMBERS // 2, n + 1 - MEMBERS // 2, n + MEMBERS // 2)
        table[k] = total_of((me_m + k) % MEMBERS)
        table_copy(k, me_m).start()
        return carry

    lax.fori_loop(0, MEMBERS - 1, send_table, 0)
    parts[me_m] = total_of(me_m)

    def got_part(k, carry):
        table_copy(k, (me_m + k) % MEMBERS).wait_recv()
        return carry

    lax.fori_loop(1, MEMBERS, got_part, 0)
    total = jnp.zeros((TOK, DIM), jnp.float32)
    for m in range(MEMBERS):
        total += parts[m].astype(jnp.float32)
    out_ref[0] = total
    for k in range(1, GROUPS):
        row_copy(k, me_g).wait_send()

    def sent_part(k, carry):
        table_copy(k, me_m).wait_send()
        return carry

    lax.fori_loop(1, MEMBERS, sent_part, 0)


def give(rows, info):
    return pl.pallas_call(
        give_kernel,
        out_shape=jax.ShapeDtypeStruct((1, TOK, DIM), jnp.float32),
        in_specs=[
            pl.BlockSpec(memory_space=pltpu.VMEM),
            pl.BlockSpec(memory_space=pltpu.SMEM),
        ],
        out_specs=pl.BlockSpec(memory_space=pltpu.VMEM),
        scratch_shapes=[
            pltpu.VMEM((GROUPS, 2 * CAP, TOK, DIM), jnp.bfloat16),
            pltpu.VMEM((MEMBERS, TOK, DIM), jnp.bfloat16),
            pltpu.VMEM((MEMBERS, TOK, DIM), jnp.bfloat16),
            pltpu.SemaphoreType.DMA((GROUPS,)),
            pltpu.SemaphoreType.DMA((GROUPS,)),
            pltpu.SemaphoreType.DMA((MEMBERS,)),
            pltpu.SemaphoreType.DMA((MEMBERS,)),
        ],
        compiler_params=pltpu.CompilerParams(collective_id=1, has_side_effects=True),
        name="give",
    )(rows, info)


def body(queries, pages, users, page_count, teacher):
    picked, lut, info = fetch(queries, users)
    scores, rows, page_grad = match(users, lut, page_count, teacher, picked, pages)
    query_grad = give(rows, info)
    return scores, query_grad, page_grad


def solution(mesh):
    both = ("group", "member")
    three, two, one = P(both, None, None), P(both, None), P(both)
    return jax.shard_map(
        body,
        mesh=mesh,
        in_specs=(three, three, two, one, two),
        out_specs=(two, three, three),
        check_vma=False,
    )
```

```python
import functools
import math

import jax
import jax.numpy as jnp
from jax import lax
from jax.experimental import pallas as pl
from jax.experimental.pallas import tpu as pltpu
from jax.sharding import PartitionSpec as P

MESH = pl.DeviceIdType.MESH
CAP = 8
GROUPS = 8
MEMBERS = 32
TOK = 32
DIM = 128
CHUNK = 8
LANES = CHUNK * TOK
INV_AT = 32
SCALE = math.log2(math.e) / 0.05
LN2 = math.log(2.0)
TOP, PEAK, MASS, MOMENT, BASE, SLANT = range(6)


def greet(me_g, me_m):
    barrier = pltpu.get_barrier_semaphore()

    def to_member(k, carry):
        pl.semaphore_signal(
            barrier, inc=1, device_id=(me_g, (me_m + k) % MEMBERS), device_id_type=MESH
        )
        return carry

    lax.fori_loop(1, MEMBERS, to_member, 0)
    for k in range(1, GROUPS):
        pl.semaphore_signal(
            barrier, inc=1, device_id=((me_g + k) % GROUPS, me_m), device_id_type=MESH
        )
    return barrier


def fetch_kernel(
    query_ref, users_ref, picked_ref, place_ref, info_ref,
    table, asks_out, asks_in, asks_smem, chosen,
    q_send, q_recv, a_send, a_recv, c_send, c_recv, local_sem,
):
    me_g = lax.axis_index("group")
    me_m = lax.axis_index("member")
    barrier = greet(me_g, me_m)

    total = GROUPS * MEMBERS
    rows = users_ref.shape[0]
    qid = lax.broadcasted_iota(jnp.int32, (total, users_ref.shape[1]), 0)
    hits = [jnp.where(users_ref[p : p + 1, :] == qid, 1.0, 0.0) for p in range(rows)]
    hit = functools.reduce(jnp.maximum, hits)
    count = lax.dot_general(
        jnp.ones((8, users_ref.shape[1]), jnp.bfloat16),
        hit.astype(jnp.bfloat16),
        (((1,), (1,)), ((), ())),
        preferred_element_type=jnp.float32,
    )
    used = jnp.where(count > 0.5, 1.0, 0.0)
    ri = lax.broadcasted_iota(jnp.int32, (total, total), 0)
    ci = lax.broadcasted_iota(jnp.int32, (total, total), 1)
    before = jnp.where((ri < ci) & ((ri >> 5) == (ci >> 5)), 1.0, 0.0).astype(jnp.bfloat16)
    rank = jnp.dot(used.astype(jnp.bfloat16), before, preferred_element_type=jnp.float32)
    lane8 = lax.broadcasted_iota(jnp.int32, (8, total), 1)
    sub8 = lax.broadcasted_iota(jnp.int32, (8, total), 0)
    spot = ((lane8 >> 5) * CAP).astype(jnp.float32) + rank
    for p in range(rows):
        place = jnp.dot(
            spot.astype(jnp.bfloat16), hits[p].astype(jnp.bfloat16),
            preferred_element_type=jnp.float32,
        )
        place_ref[p : p + 1, :] = place[0:1].astype(jnp.int32)
    of_group = (lane8 >> 5) == sub8
    k_id = lax.broadcasted_iota(jnp.int32, (128, total), 0).astype(jnp.float32)
    local_id = (lax.broadcasted_iota(jnp.int32, (128, total), 1) & 31).astype(jnp.float32)
    named = jnp.where((k_id == rank[0:1]) & (used[0:1] > 0.5), local_id, 0.0)
    ids = lax.dot_general(
        jnp.where(of_group, 1.0, 0.0).astype(jnp.bfloat16),
        named.astype(jnp.bfloat16),
        (((1,), (1,)), ((), ())),
        preferred_element_type=jnp.float32,
    )
    inverse = jnp.where(of_group, jnp.where(used > 0.5, rank, float(CAP)), 0.0)
    fold_r = lax.broadcasted_iota(jnp.int32, (total, 128), 0)
    fold_c = lax.broadcasted_iota(jnp.int32, (total, 128), 1)
    fold = jnp.where(fold_c == INV_AT + (fold_r & 31), 1.0, 0.0).astype(jnp.bfloat16)
    spread = jnp.dot(inverse.astype(jnp.bfloat16), fold, preferred_element_type=jnp.float32)
    asks = (ids + spread).astype(jnp.int32)
    for g in range(GROUPS):
        asks_out[g] = asks[g : g + 1, :]

    pl.semaphore_wait(barrier, MEMBERS - 1 + GROUPS - 1)

    def query_copy(k, src_m):
        peer = (me_m + k) % MEMBERS
        return pltpu.make_async_remote_copy(
            src_ref=query_ref.at[0],
            dst_ref=table.at[src_m],
            send_sem=q_send.at[k],
            recv_sem=q_recv.at[src_m],
            device_id=(me_g, peer),
            device_id_type=MESH,
        )

    def ask_copy(k, src_g):
        peer = (me_g + k) % GROUPS
        return pltpu.make_async_remote_copy(
            src_ref=asks_out.at[peer],
            dst_ref=asks_in.at[src_g],
            send_sem=a_send.at[k],
            recv_sem=a_recv.at[src_g],
            device_id=(peer, me_m),
            device_id_type=MESH,
        )

    def chosen_copy(k, src_g):
        peer = (me_g + k) % GROUPS
        return pltpu.make_async_remote_copy(
            src_ref=chosen.at[k],
            dst_ref=picked_ref.at[pl.ds(src_g * CAP, CAP)],
            send_sem=c_send.at[k],
            recv_sem=c_recv.at[src_g],
            device_id=(peer, me_m),
            device_id_type=MESH,
        )

    for k in range(1, GROUPS):
        ask_copy(k, me_g).start()

    def send_query(k, carry):
        query_copy(k, me_m).start()
        return carry

    lax.fori_loop(1, MEMBERS, send_query, 0)
    table[me_m] = query_ref[0]
    asks_in[me_g] = asks_out[me_g]
    for k in range(1, GROUPS):
        ask_copy(k, (me_g + k) % GROUPS).wait_recv()
    to_smem = pltpu.make_async_copy(asks_in, asks_smem, local_sem)
    to_smem.start()
    info_ref[...] = asks_in[...]
    to_smem.wait()

    def got_query(k, carry):
        query_copy(k, (me_m + k) % MEMBERS).wait_recv()
        return carry

    lax.fori_loop(1, MEMBERS, got_query, 0)
    for k in (4, 5, 2, 3, 6, 7, 1):
        peer = (me_g + k) % GROUPS
        for n in range(CAP):
            chosen[k, n] = table[asks_smem[peer, 0, n] & (MEMBERS - 1)]
        chosen_copy(k, me_g).start()
    for n in range(CAP):
        picked_ref[me_g * CAP + n] = table[asks_smem[me_g, 0, n] & (MEMBERS - 1)]
    for k in range(1, GROUPS):
        chosen_copy(k, (me_g + k) % GROUPS).wait_recv()
    for k in range(1, GROUPS):
        ask_copy(k, me_g).wait_send()
        chosen_copy(k, me_g).wait_send()

    def sent_query(k, carry):
        query_copy(k, me_m).wait_send()
        return carry

    lax.fori_loop(1, MEMBERS, sent_query, 0)


def fetch(queries, users):
    return pl.pallas_call(
        fetch_kernel,
        out_shape=(
            jax.ShapeDtypeStruct((GROUPS * CAP, TOK, DIM), jnp.bfloat16),
            jax.ShapeDtypeStruct(users.shape, jnp.int32),
            jax.ShapeDtypeStruct((GROUPS, 1, 128), jnp.int32),
        ),
        in_specs=[pl.BlockSpec(memory_space=pltpu.VMEM)] * 2,
        out_specs=[pl.BlockSpec(memory_space=pltpu.VMEM)] * 3,
        scratch_shapes=[
            pltpu.VMEM((MEMBERS, TOK, DIM), jnp.bfloat16),
            pltpu.VMEM((GROUPS, 1, 128), jnp.int32),
            pltpu.VMEM((GROUPS, 1, 128), jnp.int32),
            pltpu.SMEM((GROUPS, 1, 128), jnp.int32),
            pltpu.VMEM((GROUPS, CAP, TOK, DIM), jnp.bfloat16),
            pltpu.SemaphoreType.DMA((MEMBERS,)),
            pltpu.SemaphoreType.DMA((MEMBERS,)),
            pltpu.SemaphoreType.DMA((GROUPS,)),
            pltpu.SemaphoreType.DMA((GROUPS,)),
            pltpu.SemaphoreType.DMA((GROUPS,)),
            pltpu.SemaphoreType.DMA((GROUPS,)),
            pltpu.SemaphoreType.DMA,
        ],
        compiler_params=pltpu.CompilerParams(collective_id=0, has_side_effects=True),
        name="fetch",
    )(queries, users)


def split_dot(value, ones):
    high = value.astype(jnp.bfloat16)
    rest = value - high.astype(jnp.float32)
    mid = rest.astype(jnp.bfloat16)
    low = (rest - mid.astype(jnp.float32)).astype(jnp.bfloat16)
    dot = functools.partial(jnp.dot, preferred_element_type=jnp.float32)
    return dot(high, ones) + (dot(mid, ones) + dot(low, ones))


def match_kernel(
    place_ref, count_ref, teacher_ref, picked_hbm, pages_hbm,
    scores_ref, rows_ref, grad_hbm,
    chunks, picked_ref, pages_ref, page_t, sims, logit, expo, stats, acc, grad_ref,
    row_acc, score_l, same_slot, in_sem, out_sem,
):
    n_pages, n_tok, _ = pages_ref.shape
    per_page = place_ref.shape[1] // CHUNK
    half = n_tok // 2
    quarter = n_tok // 4

    def page_in(p):
        return pltpu.make_async_copy(pages_hbm.at[p], pages_ref.at[p], in_sem.at[p])

    picked_in = pltpu.make_async_copy(picked_hbm, picked_ref, in_sem.at[n_pages])
    for p in range(n_pages):
        page_in(p).start()
    picked_in.start()

    def list_chunk(n, total):
        p = n // per_page
        alive = (n % per_page) * CHUNK < count_ref[p]

        @pl.when(alive)
        def _():
            chunks[total] = n

        return total + alive.astype(jnp.int32)

    total = lax.fori_loop(0, n_pages * per_page, list_chunk, 0)
    for n in range(3):
        chunks[total + n] = 0
    pairs = (total + 1) // 2
    acc[...] = jnp.zeros_like(acc)
    row_acc[...] = jnp.zeros_like(row_acc)
    score_l[...] = jnp.zeros_like(score_l)
    expo[...] = jnp.zeros_like(expo)
    logit[...] = jnp.zeros_like(logit)
    stats[...] = jnp.zeros_like(stats)
    seg_r = lax.broadcasted_iota(jnp.int32, (LANES, LANES), 0) >> 5
    seg_c = lax.broadcasted_iota(jnp.int32, (LANES, LANES), 1) >> 5
    same_slot[...] = jnp.where(seg_r == seg_c, 1.0, 0.0).astype(jnp.bfloat16)
    slot_of_lane = lax.broadcasted_iota(jnp.int32, (8, LANES), 1) >> 5
    for p in range(n_pages):
        page_in(p).wait()
        page_t[p] = pages_ref[p].T
    picked_in.wait()

    def where_of(n):
        code = chunks[n]
        return code // per_page, code % per_page

    def chosen_of(p, c):
        return jnp.concatenate(
            [picked_ref[place_ref[p, c * CHUNK + k]] for k in range(CHUNK)], axis=0
        )

    def fold8(value, op):
        parts = [value[8 * i : 8 * i + 8] for i in range(value.shape[0] // 8)]
        while len(parts) > 1:
            parts = [
                op(parts[i], parts[i + 1]) if i + 1 < len(parts) else parts[i]
                for i in range(0, len(parts), 2)
            ]
        return parts[0]

    def tall(value, rows):
        return jnp.concatenate([value] * (rows // 8), axis=0)

    def similar_half(p, chosen, slot, h):
        at = slice(half * h, half * h + half)
        block = lax.dot_general(
            pages_ref[p, at, :], chosen, (((1,), (1,)), ((), ())),
            preferred_element_type=jnp.float32,
        )
        sims[slot, at, :] = block
        return fold8(block, jnp.maximum)

    def similar(n, slot):
        p, c = where_of(n)
        chosen = chosen_of(p, c)
        tops = [similar_half(p, chosen, slot, h) for h in range(2)]
        stats[slot, TOP] = jnp.maximum(*tops)

    def weigh_rows(slot, top, start, rows):
        mass = moment = None
        for i in range(rows // 32):
            at = slice(start + 32 * i, start + 32 * i + 32)
            t = sims[slot, at, :] * SCALE - tall(top, 32)
            e = jnp.exp2(t)
            g = e * t
            logit[slot, at, :] = t
            expo[slot, at, :] = e
            e, g = fold8(e, jnp.add), fold8(g, jnp.add)
            mass = e if mass is None else mass + e
            moment = g if moment is None else moment + g
        return mass, moment

    def settle(n, slot):
        p, c = where_of(n)
        known = n < total
        mass = jnp.broadcast_to(
            jnp.sum(stats[slot, MASS], axis=0, keepdims=True), (8, LANES)
        )
        moment = jnp.broadcast_to(
            jnp.sum(stats[slot, MOMENT], axis=0, keepdims=True), (8, LANES)
        )
        mean = moment / mass
        matched = (stats[slot, PEAK] + mean) * (1.0 / SCALE)
        score = split_dot(matched, same_slot[...])
        taught = jnp.zeros((8, LANES), jnp.float32)
        for k in range(CHUNK):
            taught = jnp.where(slot_of_lane == k, teacher_ref[p, c * CHUNK + k], taught)
        bound = jnp.where(known, count_ref[p] - c * CHUNK, 0)
        live = slot_of_lane < bound
        row = jnp.where(known, p, n_pages)
        score_l[c, pl.ds(row, 1), :] = jnp.where(live, score, 0.0)[0:1]
        part = jnp.where(live, (score - taught) / mass, 0.0)
        slant = part * LN2
        stats[slot, BASE] = part - slant * mean
        stats[slot, SLANT] = slant

    def slope_rows(slot, base, slant, start, rows):
        parts = []
        for i in range(rows // 32):
            at = slice(start + 32 * i, start + 32 * i + 32)
            parts.append(
                (
                    expo[slot, at, :] * (tall(base, 32) + tall(slant, 32) * logit[slot, at, :])
                ).astype(jnp.bfloat16)
            )
        return jnp.concatenate(parts, axis=0)

    def spread_rows(p, chosen, slope, at, query_t):
        acc[p, at, :] += jnp.dot(slope, chosen, preferred_element_type=jnp.float32)
        part = jnp.dot(page_t[p, :, at], slope, preferred_element_type=jnp.float32)
        return part if query_t is None else query_t + part

    def add_rows(p, c, query_t):
        query_part = query_t.T
        for k in range(CHUNK):
            row_acc[place_ref[p, c * CHUNK + k]] += query_part[TOK * k : TOK * k + TOK]

    def spread(n, slot):
        p, c = where_of(n)
        chosen = chosen_of(p, c)
        base, slant = stats[slot, BASE], stats[slot, SLANT]
        query_t = None
        for b in range(4):
            at = slice(quarter * b, quarter * b + quarter)
            slope = slope_rows(slot, base, slant, quarter * b, quarter)
            query_t = spread_rows(p, chosen, slope, at, query_t)
        add_rows(p, c, query_t)

    def turn(old, now, new, slot):
        p_old, c_old = where_of(old)
        p_new, c_new = where_of(new)
        chosen_old = chosen_of(p_old, c_old)
        chosen_new = chosen_of(p_new, c_new)
        base, slant = stats[slot, BASE], stats[slot, SLANT]
        top = jnp.broadcast_to(
            jnp.max(stats[slot, TOP], axis=0, keepdims=True), (8, LANES)
        ) * SCALE
        stats[slot, PEAK] = top
        query_t = mass = moment = None
        tops = []
        for h in range(2):
            for b in (2 * h, 2 * h + 1):
                at = slice(quarter * b, quarter * b + quarter)
                slope = slope_rows(slot, base, slant, quarter * b, quarter)
                query_t = spread_rows(p_old, chosen_old, slope, at, query_t)
                e, g = weigh_rows(slot, top, quarter * b, quarter)
                mass = e if mass is None else mass + e
                moment = g if moment is None else moment + g
            tops.append(similar_half(p_new, chosen_new, slot, h))
        stats[slot, TOP] = jnp.maximum(*tops)
        stats[slot, MASS] = mass
        stats[slot, MOMENT] = moment
        add_rows(p_old, c_old, query_t)

    similar(0, 0)
    similar(1, 1)

    def step(i, carry):
        n = 2 * i
        old = jnp.maximum(n - 2, 0)

        turn(old, n, n + 2, 0)
        settle(n, 0)
        turn(old + 1, n + 1, n + 3, 1)
        settle(n + 1, 1)
        return carry

    lax.fori_loop(0, pairs, step, 0)
    spread(2 * pairs - 2, 0)
    spread(2 * pairs - 1, 1)

    def page_out(p):
        return pltpu.make_async_copy(grad_ref.at[p], grad_hbm.at[p], out_sem.at[p])

    for p in range(n_pages):
        grad_ref[p] = acc[p].astype(jnp.bfloat16)
        page_out(p).start()
    col = lax.broadcasted_iota(jnp.int32, (LANES, 128), 1)
    row = lax.broadcasted_iota(jnp.int32, (LANES, 128), 0)
    out = jnp.zeros((8, 128), jnp.float32)
    for c in range(per_page):
        take = jnp.where(row == (col - c * CHUNK) * TOK, 1.0, 0.0)
        out += split_dot(score_l[c], take.astype(jnp.bfloat16))
    scores_ref[...] = out[: scores_ref.shape[0], : scores_ref.shape[1]]
    rows_ref[...] = row_acc[...].astype(jnp.bfloat16)
    for p in range(n_pages):
        page_out(p).wait()


def match(place, page_count, teacher, picked, pages):
    n_pages, n_tok, _ = pages.shape
    per_page = teacher.shape[1] // CHUNK
    smem = pl.BlockSpec(memory_space=pltpu.SMEM)
    vmem = pl.BlockSpec(memory_space=pltpu.VMEM)
    anywhere = pl.BlockSpec(memory_space=pl.ANY)
    return pl.pallas_call(
        match_kernel,
        out_shape=(
            jax.ShapeDtypeStruct(teacher.shape, jnp.float32),
            jax.ShapeDtypeStruct(picked.shape, jnp.bfloat16),
            jax.ShapeDtypeStruct(pages.shape, jnp.bfloat16),
        ),
        in_specs=[smem, smem, smem, anywhere, anywhere],
        out_specs=[vmem, vmem, anywhere],
        scratch_shapes=[
            pltpu.SMEM((n_pages * per_page + 3,), jnp.int32),
            pltpu.VMEM(picked.shape, jnp.bfloat16),
            pltpu.VMEM(pages.shape, jnp.bfloat16),
            pltpu.VMEM((n_pages, DIM, n_tok), jnp.bfloat16),
            pltpu.VMEM((2, n_tok, LANES), jnp.float32),
            pltpu.VMEM((2, n_tok, LANES), jnp.float32),
            pltpu.VMEM((2, n_tok, LANES), jnp.float32),
            pltpu.VMEM((2, 6, 8, LANES), jnp.float32),
            pltpu.VMEM((n_pages, n_tok, DIM), jnp.float32),
            pltpu.VMEM(pages.shape, jnp.bfloat16),
            pltpu.VMEM(picked.shape, jnp.float32),
            pltpu.VMEM((per_page, 8, LANES), jnp.float32),
            pltpu.VMEM((LANES, LANES), jnp.bfloat16),
            pltpu.SemaphoreType.DMA((n_pages + 1,)),
            pltpu.SemaphoreType.DMA((n_pages,)),
        ],
        compiler_params=pltpu.CompilerParams(vmem_limit_bytes=60 * 1024 * 1024),
        name="match",
    )(place, page_count, teacher, picked, pages)


def give_kernel(
    rows_ref, info_ref, out_ref,
    landed, table, parts, r_send, r_recv, t_send, t_recv,
):
    me_g = lax.axis_index("group")
    me_m = lax.axis_index("member")
    barrier = greet(me_g, me_m)
    for s in range(GROUPS):
        for spare in range(CAP, 2 * CAP):
            landed[s, spare] = jnp.zeros((TOK, DIM), jnp.bfloat16)
    pl.semaphore_wait(barrier, MEMBERS - 1 + GROUPS - 1)

    def row_copy(k, src_g):
        peer = (me_g + k) % GROUPS
        return pltpu.make_async_remote_copy(
            src_ref=rows_ref.at[pl.ds(peer * CAP, CAP)],
            dst_ref=landed.at[src_g, pl.ds(0, CAP)],
            send_sem=r_send.at[k],
            recv_sem=r_recv.at[src_g],
            device_id=(peer, me_m),
            device_id_type=MESH,
        )

    def table_copy(k, src_m):
        peer = (me_m + k) % MEMBERS
        return pltpu.make_async_remote_copy(
            src_ref=table.at[k],
            dst_ref=parts.at[src_m],
            send_sem=t_send.at[k],
            recv_sem=t_recv.at[src_m],
            device_id=(me_g, peer),
            device_id_type=MESH,
        )

    for k in (4, 5, 2, 3, 6, 7, 1):
        row_copy(k, me_g).start()
    for n in range(CAP):
        landed[me_g, n] = rows_ref[me_g * CAP + n]
    for k in range(1, GROUPS):
        row_copy(k, (me_g + k) % GROUPS).wait_recv()

    def total_of(owner):
        total = jnp.zeros((TOK, DIM), jnp.float32)
        for s in range(GROUPS):
            total += landed[s, info_ref[s, 0, INV_AT + owner] & (2 * CAP - 1)].astype(jnp.float32)
        return total.astype(jnp.bfloat16)

    def send_table(n, carry):
        k = jnp.where(n >= MEMBERS // 2, n + 1 - MEMBERS // 2, n + MEMBERS // 2)
        table[k] = total_of((me_m + k) % MEMBERS)
        table_copy(k, me_m).start()
        return carry

    lax.fori_loop(0, MEMBERS - 1, send_table, 0)
    parts[me_m] = total_of(me_m)

    def got_part(k, carry):
        table_copy(k, (me_m + k) % MEMBERS).wait_recv()
        return carry

    lax.fori_loop(1, MEMBERS, got_part, 0)
    total = jnp.zeros((TOK, DIM), jnp.float32)
    for m in range(MEMBERS):
        total += parts[m].astype(jnp.float32)
    out_ref[0] = total
    for k in range(1, GROUPS):
        row_copy(k, me_g).wait_send()

    def sent_part(k, carry):
        table_copy(k, me_m).wait_send()
        return carry

    lax.fori_loop(1, MEMBERS, sent_part, 0)


def give(rows, info):
    return pl.pallas_call(
        give_kernel,
        out_shape=jax.ShapeDtypeStruct((1, TOK, DIM), jnp.float32),
        in_specs=[
            pl.BlockSpec(memory_space=pltpu.VMEM),
            pl.BlockSpec(memory_space=pltpu.SMEM),
        ],
        out_specs=pl.BlockSpec(memory_space=pltpu.VMEM),
        scratch_shapes=[
            pltpu.VMEM((GROUPS, 2 * CAP, TOK, DIM), jnp.bfloat16),
            pltpu.VMEM((MEMBERS, TOK, DIM), jnp.bfloat16),
            pltpu.VMEM((MEMBERS, TOK, DIM), jnp.bfloat16),
            pltpu.SemaphoreType.DMA((GROUPS,)),
            pltpu.SemaphoreType.DMA((GROUPS,)),
            pltpu.SemaphoreType.DMA((MEMBERS,)),
            pltpu.SemaphoreType.DMA((MEMBERS,)),
        ],
        compiler_params=pltpu.CompilerParams(collective_id=1, has_side_effects=True),
        name="give",
    )(rows, info)


def body(queries, pages, users, page_count, teacher):
    picked, place, info = fetch(queries, users)
    scores, rows, page_grad = match(place, page_count, teacher, picked, pages)
    query_grad = give(rows, info)
    return scores, query_grad, page_grad


def solution(mesh):
    both = ("group", "member")
    three, two, one = P(both, None, None), P(both, None), P(both)
    return jax.shard_map(
        body,
        mesh=mesh,
        in_specs=(three, three, two, one, two),
        out_specs=(two, three, three),
        check_vma=False,
    )
```

```python
import functools
import math

import jax
import jax.numpy as jnp
from jax import lax
from jax.experimental import pallas as pl
from jax.experimental.pallas import tpu as pltpu
from jax.sharding import PartitionSpec as P

MESH = pl.DeviceIdType.MESH
CAP = 8
GROUPS = 8
MEMBERS = 32
TOK = 32
ZS, YS = 8, 4
Z_FAR = (4, 3, 5, 2, 6, 1, 7)
Z_NEAR = (1, 7, 2, 6, 3, 5, 4)
Y_FAR = (2, 1, 3)
DIM = 128
CHUNK = 8
LANES = CHUNK * TOK
INV_AT = 32
SCALE = math.log2(math.e) / 0.05
LN2 = math.log(2.0)
TOP, PEAK, MASS, MOMENT, BASE, SLANT = range(6)


def along(me_m, dz, dy):
    return ((me_m // YS + dz) % ZS) * YS + (me_m % YS + dy) % YS


def greet(me_g, me_m):
    barrier = pltpu.get_barrier_semaphore()
    peers = [(me_g, along(me_m, k, 0)) for k in Z_FAR]
    peers += [(me_g, along(me_m, 0, k)) for k in range(1, YS)]
    peers += [((me_g + k) % GROUPS, me_m) for k in range(1, GROUPS)]
    for peer in peers:
        pl.semaphore_signal(barrier, inc=1, device_id=peer, device_id_type=MESH)
    return barrier, len(peers)


def fetch_kernel(
    query_hbm, users_hbm, pages_hbm, picked_hbm, place_ref, info_ref, page_t_hbm,
    table, users_ref, pages_ref, page_t, asks_out, asks_in, asks_smem, chosen,
    z_send, y_send, q_recv, a_send, a_recv, c_send, c_recv, local_sem, in_sem, out_sem,
):
    me_g = lax.axis_index("group")
    me_m = lax.axis_index("member")
    n_pages = pages_hbm.shape[0]
    barrier, greeted = greet(me_g, me_m)
    users_in = pltpu.make_async_copy(users_hbm, users_ref, local_sem.at[0])
    query_in = pltpu.make_async_copy(query_hbm.at[0], table.at[me_m], local_sem.at[1])
    users_in.start()
    query_in.start()

    def page_in(p):
        return pltpu.make_async_copy(pages_hbm.at[p], pages_ref.at[p], in_sem.at[p])

    def page_out(p):
        return pltpu.make_async_copy(page_t.at[p], page_t_hbm.at[p], out_sem.at[p])

    for p in range(n_pages):
        page_in(p).start()
    users_in.wait()

    total = GROUPS * MEMBERS
    rows = users_ref.shape[0]
    qid = lax.broadcasted_iota(jnp.int32, (total, users_ref.shape[1]), 0)
    hits = [jnp.where(users_ref[p : p + 1, :] == qid, 1.0, 0.0) for p in range(rows)]
    hit = functools.reduce(jnp.maximum, hits)
    count = lax.dot_general(
        jnp.ones((8, users_ref.shape[1]), jnp.bfloat16),
        hit.astype(jnp.bfloat16),
        (((1,), (1,)), ((), ())),
        preferred_element_type=jnp.float32,
    )
    used = jnp.where(count > 0.5, 1.0, 0.0)
    ri = lax.broadcasted_iota(jnp.int32, (total, total), 0)
    ci = lax.broadcasted_iota(jnp.int32, (total, total), 1)
    before = jnp.where((ri < ci) & ((ri >> 5) == (ci >> 5)), 1.0, 0.0).astype(jnp.bfloat16)
    rank = jnp.dot(used.astype(jnp.bfloat16), before, preferred_element_type=jnp.float32)
    lane8 = lax.broadcasted_iota(jnp.int32, (8, total), 1)
    sub8 = lax.broadcasted_iota(jnp.int32, (8, total), 0)
    of_group = (lane8 >> 5) == sub8
    k_id = lax.broadcasted_iota(jnp.int32, (128, total), 0).astype(jnp.float32)
    local_id = (lax.broadcasted_iota(jnp.int32, (128, total), 1) & 31).astype(jnp.float32)
    named = jnp.where((k_id == rank[0:1]) & (used[0:1] > 0.5), local_id, 0.0)
    ids = lax.dot_general(
        jnp.where(of_group, 1.0, 0.0).astype(jnp.bfloat16),
        named.astype(jnp.bfloat16),
        (((1,), (1,)), ((), ())),
        preferred_element_type=jnp.float32,
    )
    inverse = jnp.where(of_group, jnp.where(used > 0.5, rank, float(CAP)), 0.0)
    fold_r = lax.broadcasted_iota(jnp.int32, (total, 128), 0)
    fold_c = lax.broadcasted_iota(jnp.int32, (total, 128), 1)
    fold = jnp.where(fold_c == INV_AT + (fold_r & 31), 1.0, 0.0).astype(jnp.bfloat16)
    spread = jnp.dot(inverse.astype(jnp.bfloat16), fold, preferred_element_type=jnp.float32)
    asks = (ids + spread).astype(jnp.int32)
    for g in range(GROUPS):
        asks_out[g] = asks[g : g + 1, :]
    query_in.wait()

    def remote(src, dst, send, recv, g, m):
        return pltpu.make_async_remote_copy(
            src_ref=src, dst_ref=dst, send_sem=send, recv_sem=recv,
            device_id=(g, m), device_id_type=MESH,
        )

    def z_copy(k, src_m):
        return remote(
            table.at[src_m], table.at[src_m], z_send.at[k], q_recv.at[src_m],
            me_g, along(me_m, k, 0),
        )

    def y_copy(k, j, src_m):
        return remote(
            table.at[src_m], table.at[src_m], y_send.at[YS * k + j], q_recv.at[src_m],
            me_g, along(me_m, 0, j),
        )

    def ask_copy(k, src_g):
        peer = (me_g + k) % GROUPS
        return remote(
            asks_out.at[peer], asks_in.at[src_g], a_send.at[k], a_recv.at[src_g], peer, me_m
        )

    def chosen_copy(k, src_g):
        peer = (me_g + k) % GROUPS
        return remote(
            chosen.at[k], picked_hbm.at[pl.ds(src_g * CAP, CAP)],
            c_send.at[k], c_recv.at[src_g], peer, me_m,
        )

    pl.semaphore_wait(barrier, greeted)
    for k in Z_FAR:
        z_copy(k, me_m).start()
    for j in Y_FAR:
        y_copy(0, j, me_m).start()
    for k in range(1, GROUPS):
        ask_copy(k, me_g).start()
    asks_in[me_g] = asks_out[me_g]
    spot = ((lane8 >> 5) * CAP).astype(jnp.float32) + rank
    for p in range(rows):
        place = jnp.dot(
            spot.astype(jnp.bfloat16), hits[p].astype(jnp.bfloat16),
            preferred_element_type=jnp.float32,
        )
        place_ref[p : p + 1, :] = place[0:1].astype(jnp.int32)
    for p in range(n_pages):
        page_in(p).wait()
        page_t[p] = pages_ref[p].T
        page_out(p).start()
    for k in Z_NEAR:
        src = along(me_m, k, 0)
        z_copy(k, src).wait_recv()
        for j in Y_FAR:
            y_copy(k, j, src).start()
    for k in range(1, GROUPS):
        ask_copy(k, (me_g + k) % GROUPS).wait_recv()
    to_smem = pltpu.make_async_copy(asks_in, asks_smem, local_sem.at[0])
    to_smem.start()
    info_ref[...] = asks_in[...]
    to_smem.wait()
    for k in (0,) + Z_NEAR:
        for j in range(1, YS):
            y_copy(k, j, along(me_m, k, j)).wait_recv()

    for k in (4, 5, 2, 3, 6, 7, 1, 0):
        peer = (me_g + k) % GROUPS
        for n in range(CAP):
            chosen[k, n] = table[asks_smem[peer, 0, n] & (MEMBERS - 1)]
        if k:
            chosen_copy(k, me_g).start()
    own = pltpu.make_async_copy(
        chosen.at[0], picked_hbm.at[pl.ds(me_g * CAP, CAP)], local_sem.at[1]
    )
    own.start()
    for p in range(n_pages):
        page_out(p).wait()
    for k in Z_NEAR:
        z_copy(k, me_m).wait_send()
    for k in (0,) + Z_NEAR:
        for j in range(1, YS):
            y_copy(k, j, along(me_m, k, 0)).wait_send()
    own.wait()
    for k in range(1, GROUPS):
        chosen_copy(k, (me_g + k) % GROUPS).wait_recv()
        ask_copy(k, me_g).wait_send()
        chosen_copy(k, me_g).wait_send()


def fetch(queries, users, pages):
    n_pages, n_tok, _ = pages.shape
    vmem = pl.BlockSpec(memory_space=pltpu.VMEM)
    anywhere = pl.BlockSpec(memory_space=pl.ANY)
    return pl.pallas_call(
        fetch_kernel,
        out_shape=(
            jax.ShapeDtypeStruct((GROUPS * CAP, TOK, DIM), jnp.bfloat16),
            jax.ShapeDtypeStruct(users.shape, jnp.int32),
            jax.ShapeDtypeStruct((GROUPS, 1, 128), jnp.int32),
            jax.ShapeDtypeStruct((n_pages, DIM, n_tok), jnp.bfloat16),
        ),
        in_specs=[anywhere] * 3,
        out_specs=[anywhere, vmem, vmem, anywhere],
        scratch_shapes=[
            pltpu.VMEM((MEMBERS, TOK, DIM), jnp.bfloat16),
            pltpu.VMEM(users.shape, jnp.int32),
            pltpu.VMEM(pages.shape, jnp.bfloat16),
            pltpu.VMEM((n_pages, DIM, n_tok), jnp.bfloat16),
            pltpu.VMEM((GROUPS, 1, 128), jnp.int32),
            pltpu.VMEM((GROUPS, 1, 128), jnp.int32),
            pltpu.SMEM((GROUPS, 1, 128), jnp.int32),
            pltpu.VMEM((GROUPS, CAP, TOK, DIM), jnp.bfloat16),
            pltpu.SemaphoreType.DMA((ZS,)),
            pltpu.SemaphoreType.DMA((MEMBERS,)),
            pltpu.SemaphoreType.DMA((MEMBERS,)),
            pltpu.SemaphoreType.DMA((GROUPS,)),
            pltpu.SemaphoreType.DMA((GROUPS,)),
            pltpu.SemaphoreType.DMA((GROUPS,)),
            pltpu.SemaphoreType.DMA((GROUPS,)),
            pltpu.SemaphoreType.DMA((2,)),
            pltpu.SemaphoreType.DMA((n_pages,)),
            pltpu.SemaphoreType.DMA((n_pages,)),
        ],
        compiler_params=pltpu.CompilerParams(
            collective_id=0, has_side_effects=True, vmem_limit_bytes=60 * 1024 * 1024
        ),
        name="fetch",
    )(queries, users, pages)


def split_dot(value, ones):
    high = value.astype(jnp.bfloat16)
    rest = value - high.astype(jnp.float32)
    mid = rest.astype(jnp.bfloat16)
    low = (rest - mid.astype(jnp.float32)).astype(jnp.bfloat16)
    dot = functools.partial(jnp.dot, preferred_element_type=jnp.float32)
    return dot(high, ones) + (dot(mid, ones) + dot(low, ones))


def match_kernel(
    place_ref, count_ref, teacher_ref, picked_hbm, pages_hbm, page_t_hbm,
    scores_ref, rows_ref, grad_hbm,
    chunks, picked_ref, scaled, pages_ref, page_t, sims, logit, expo, stats, acc,
    grad_ref, row_acc, score_l, same_slot, in_sem, out_sem,
):
    n_pages, n_tok, _ = pages_ref.shape
    per_page = place_ref.shape[1] // CHUNK
    half = n_tok // 2
    quarter = n_tok // 4

    def page_in(p):
        return pltpu.make_async_copy(pages_hbm.at[p], pages_ref.at[p], in_sem.at[p])

    picked_in = pltpu.make_async_copy(picked_hbm, picked_ref, in_sem.at[n_pages])
    turned_in = pltpu.make_async_copy(page_t_hbm, page_t, in_sem.at[n_pages + 1])
    picked_in.start()
    for p in range(n_pages):
        page_in(p).start()
    turned_in.start()

    def list_chunk(n, total):
        p = n // per_page
        alive = (n % per_page) * CHUNK < count_ref[p]

        @pl.when(alive)
        def _():
            chunks[total] = n

        return total + alive.astype(jnp.int32)

    total = lax.fori_loop(0, n_pages * per_page, list_chunk, 0)
    for n in range(3):
        chunks[total + n] = 0
    pairs = (total + 1) // 2
    acc[...] = jnp.zeros_like(acc)
    row_acc[...] = jnp.zeros_like(row_acc)
    score_l[...] = jnp.zeros_like(score_l)
    expo[...] = jnp.zeros_like(expo)
    logit[...] = jnp.zeros_like(logit)
    stats[...] = jnp.zeros_like(stats)
    seg_r = lax.broadcasted_iota(jnp.int32, (LANES, LANES), 0) >> 5
    seg_c = lax.broadcasted_iota(jnp.int32, (LANES, LANES), 1) >> 5
    same_slot[...] = jnp.where(seg_r == seg_c, 1.0, 0.0).astype(jnp.bfloat16)
    slot_of_lane = lax.broadcasted_iota(jnp.int32, (8, LANES), 1) >> 5
    picked_in.wait()

    def scale_picked(n, carry):
        full = picked_ref[n].astype(jnp.float32) * SCALE
        high = full.astype(jnp.bfloat16)
        scaled[n, :, :DIM] = high
        scaled[n, :, DIM:] = (full - high.astype(jnp.float32)).astype(jnp.bfloat16)
        return carry

    lax.fori_loop(0, picked_ref.shape[0], scale_picked, 0, unroll=8)
    for p in range(n_pages):
        page_in(p).wait()
    turned_in.wait()

    def where_of(n):
        code = chunks[n]
        return code // per_page, code % per_page

    def chosen_of(p, c, source):
        return jnp.concatenate(
            [source[place_ref[p, c * CHUNK + k]] for k in range(CHUNK)], axis=0
        )

    def fold8(value, op):
        parts = [value[8 * i : 8 * i + 8] for i in range(value.shape[0] // 8)]
        while len(parts) > 1:
            parts = [
                op(parts[i], parts[i + 1]) if i + 1 < len(parts) else parts[i]
                for i in range(0, len(parts), 2)
            ]
        return parts[0]

    def tall(value, rows):
        return jnp.concatenate([value] * (rows // 8), axis=0)

    def similar_half(p, chosen, slot, h):
        at = slice(half * h, half * h + half)
        page = pages_ref[p, at, :]
        block = lax.dot_general(
            jnp.concatenate([page, page], axis=1), chosen, (((1,), (1,)), ((), ())),
            preferred_element_type=jnp.float32,
        )
        sims[slot, at, :] = block
        return fold8(block, jnp.maximum)

    def similar(n, slot):
        p, c = where_of(n)
        chosen = chosen_of(p, c, scaled)
        tops = [similar_half(p, chosen, slot, h) for h in range(2)]
        stats[slot, TOP] = jnp.maximum(*tops)

    def weigh_rows(slot, top, start, rows):
        mass = moment = None
        for i in range(rows // 32):
            at = slice(start + 32 * i, start + 32 * i + 32)
            t = sims[slot, at, :] - tall(top, 32)
            e = jnp.exp2(t)
            g = e * t
            logit[slot, at, :] = t
            expo[slot, at, :] = e
            e, g = fold8(e, jnp.add), fold8(g, jnp.add)
            mass = e if mass is None else mass + e
            moment = g if moment is None else moment + g
        return mass, moment

    def settle(n, slot):
        p, c = where_of(n)
        known = n < total
        mass = jnp.broadcast_to(
            jnp.sum(stats[slot, MASS], axis=0, keepdims=True), (8, LANES)
        )
        moment = jnp.broadcast_to(
            jnp.sum(stats[slot, MOMENT], axis=0, keepdims=True), (8, LANES)
        )
        mean = moment / mass
        matched = (stats[slot, PEAK] + mean) * (1.0 / SCALE)
        score = split_dot(matched, same_slot[...])
        taught = jnp.zeros((8, LANES), jnp.float32)
        for k in range(CHUNK):
            taught = jnp.where(slot_of_lane == k, teacher_ref[p, c * CHUNK + k], taught)
        bound = jnp.where(known, count_ref[p] - c * CHUNK, 0)
        live = slot_of_lane < bound
        row = jnp.where(known, p, n_pages)
        score_l[c, pl.ds(row, 1), :] = jnp.where(live, score, 0.0)[0:1]
        part = jnp.where(live, (score - taught) / mass, 0.0)
        slant = part * LN2
        stats[slot, BASE] = part - slant * mean
        stats[slot, SLANT] = slant

    def slope_rows(slot, base, slant, start, rows):
        parts = []
        for i in range(rows // 32):
            at = slice(start + 32 * i, start + 32 * i + 32)
            t = logit[slot, at, :]
            parts.append(
                (expo[slot, at, :] * (tall(base, 32) + tall(slant, 32) * t)).astype(jnp.bfloat16)
            )
        return jnp.concatenate(parts, axis=0)

    def spread_rows(p, chosen, slope, at, query_t):
        acc[p, at, :] += jnp.dot(slope, chosen, preferred_element_type=jnp.float32)
        part = jnp.dot(page_t[p, :, at], slope, preferred_element_type=jnp.float32)
        return part if query_t is None else query_t + part

    def add_rows(p, c, query_t):
        query_part = query_t.T
        for k in range(CHUNK):
            row_acc[place_ref[p, c * CHUNK + k]] += query_part[TOK * k : TOK * k + TOK]

    def spread(n, slot):
        p, c = where_of(n)
        chosen = chosen_of(p, c, picked_ref)
        base, slant = stats[slot, BASE], stats[slot, SLANT]
        query_t = None
        for b in range(4):
            at = slice(quarter * b, quarter * b + quarter)
            slope = slope_rows(slot, base, slant, quarter * b, quarter)
            query_t = spread_rows(p, chosen, slope, at, query_t)
        add_rows(p, c, query_t)

    def turn(old, now, new, slot):
        p_old, c_old = where_of(old)
        p_new, c_new = where_of(new)
        chosen_old = chosen_of(p_old, c_old, picked_ref)
        chosen_new = chosen_of(p_new, c_new, scaled)
        base, slant = stats[slot, BASE], stats[slot, SLANT]
        top = jnp.broadcast_to(
            jnp.max(stats[slot, TOP], axis=0, keepdims=True), (8, LANES)
        )
        stats[slot, PEAK] = top
        query_t = mass = moment = None
        tops = []
        for h in range(2):
            for b in (2 * h, 2 * h + 1):
                at = slice(quarter * b, quarter * b + quarter)
                slope = slope_rows(slot, base, slant, quarter * b, quarter)
                query_t = spread_rows(p_old, chosen_old, slope, at, query_t)
                e, g = weigh_rows(slot, top, quarter * b, quarter)
                mass = e if mass is None else mass + e
                moment = g if moment is None else moment + g
            tops.append(similar_half(p_new, chosen_new, slot, h))
        stats[slot, TOP] = jnp.maximum(*tops)
        stats[slot, MASS] = mass
        stats[slot, MOMENT] = moment
        add_rows(p_old, c_old, query_t)

    similar(0, 0)
    similar(1, 1)

    def step(i, carry):
        n = 2 * i
        old = jnp.maximum(n - 2, 0)

        turn(old, n, n + 2, 0)
        settle(n, 0)
        turn(old + 1, n + 1, n + 3, 1)
        settle(n + 1, 1)
        return carry

    lax.fori_loop(0, pairs, step, 0)
    spread(2 * pairs - 2, 0)
    spread(2 * pairs - 1, 1)

    def page_out(p):
        return pltpu.make_async_copy(grad_ref.at[p], grad_hbm.at[p], out_sem.at[p])

    for p in range(n_pages):
        grad_ref[p] = acc[p].astype(jnp.bfloat16)
        page_out(p).start()
    col = lax.broadcasted_iota(jnp.int32, (LANES, 128), 1)
    row = lax.broadcasted_iota(jnp.int32, (LANES, 128), 0)
    out = jnp.zeros((8, 128), jnp.float32)
    for c in range(per_page):
        take = jnp.where(row == (col - c * CHUNK) * TOK, 1.0, 0.0)
        out += split_dot(score_l[c], take.astype(jnp.bfloat16))
    scores_ref[...] = out[: scores_ref.shape[0], : scores_ref.shape[1]]
    rows_ref[...] = row_acc[...].astype(jnp.bfloat16)
    for p in range(n_pages):
        page_out(p).wait()


def match(place, page_count, teacher, picked, pages, page_t):
    n_pages, n_tok, _ = pages.shape
    per_page = teacher.shape[1] // CHUNK
    smem = pl.BlockSpec(memory_space=pltpu.SMEM)
    vmem = pl.BlockSpec(memory_space=pltpu.VMEM)
    anywhere = pl.BlockSpec(memory_space=pl.ANY)
    return pl.pallas_call(
        match_kernel,
        out_shape=(
            jax.ShapeDtypeStruct(teacher.shape, jnp.float32),
            jax.ShapeDtypeStruct(picked.shape, jnp.bfloat16),
            jax.ShapeDtypeStruct(pages.shape, jnp.bfloat16),
        ),
        in_specs=[smem, smem, smem, anywhere, anywhere, anywhere],
        out_specs=[vmem, vmem, anywhere],
        scratch_shapes=[
            pltpu.SMEM((n_pages * per_page + 3,), jnp.int32),
            pltpu.VMEM(picked.shape, jnp.bfloat16),
            pltpu.VMEM((GROUPS * CAP, TOK, 2 * DIM), jnp.bfloat16),
            pltpu.VMEM(pages.shape, jnp.bfloat16),
            pltpu.VMEM((n_pages, DIM, n_tok), jnp.bfloat16),
            pltpu.VMEM((2, n_tok, LANES), jnp.float32),
            pltpu.VMEM((2, n_tok, LANES), jnp.float32),
            pltpu.VMEM((2, n_tok, LANES), jnp.float32),
            pltpu.VMEM((2, 6, 8, LANES), jnp.float32),
            pltpu.VMEM((n_pages, n_tok, DIM), jnp.float32),
            pltpu.VMEM(pages.shape, jnp.bfloat16),
            pltpu.VMEM(picked.shape, jnp.float32),
            pltpu.VMEM((per_page, 8, LANES), jnp.float32),
            pltpu.VMEM((LANES, LANES), jnp.bfloat16),
            pltpu.SemaphoreType.DMA((n_pages + 2,)),
            pltpu.SemaphoreType.DMA((n_pages,)),
        ],
        compiler_params=pltpu.CompilerParams(vmem_limit_bytes=60 * 1024 * 1024),
        name="match",
    )(place, page_count, teacher, picked, pages, page_t)


def give_kernel(
    rows_hbm, info_ref, out_ref,
    rows_ref, landed, table, y_parts, z_sums, z_parts,
    r_send, r_recv, y_send, y_recv, z_send, z_recv, local_sem,
):
    me_g = lax.axis_index("group")
    me_m = lax.axis_index("member")
    barrier, greeted = greet(me_g, me_m)
    rows_in = pltpu.make_async_copy(rows_hbm, rows_ref, local_sem)
    rows_in.start()
    for s in range(GROUPS):
        for spare in range(CAP, 2 * CAP):
            landed[s, spare] = jnp.zeros((TOK, DIM), jnp.bfloat16)
    rows_in.wait()
    for n in range(CAP):
        landed[me_g, n] = rows_ref[me_g * CAP + n]
    pl.semaphore_wait(barrier, greeted)

    def remote(src, dst, send, recv, g, m):
        return pltpu.make_async_remote_copy(
            src_ref=src, dst_ref=dst, send_sem=send, recv_sem=recv,
            device_id=(g, m), device_id_type=MESH,
        )

    def row_copy(k, src_g):
        peer = (me_g + k) % GROUPS
        return remote(
            rows_ref.at[pl.ds(peer * CAP, CAP)], landed.at[src_g, pl.ds(0, CAP)],
            r_send.at[k], r_recv.at[src_g], peer, me_m,
        )

    def y_copy(k, j, slot):
        return remote(
            table.at[YS * k + j], y_parts.at[YS * k + slot],
            y_send.at[YS * k + j], y_recv.at[YS * k + slot], me_g, along(me_m, 0, j),
        )

    def z_copy(k, slot):
        return remote(
            z_sums.at[k], z_parts.at[slot], z_send.at[k], z_recv.at[slot],
            me_g, along(me_m, k, 0),
        )

    for k in (4, 5, 2, 3, 6, 7, 1):
        row_copy(k, me_g).start()
    for k in range(1, GROUPS):
        row_copy(k, (me_g + k) % GROUPS).wait_recv()

    def total_of(owner):
        total = jnp.zeros((TOK, DIM), jnp.float32)
        for s in range(GROUPS):
            total += landed[s, info_ref[s, 0, INV_AT + owner] & (2 * CAP - 1)].astype(
                jnp.float32
            )
        return total

    for k in Z_FAR + (0,):
        for j in Y_FAR:
            table[YS * k + j] = total_of(along(me_m, k, j)).astype(jnp.bfloat16)
            y_copy(k, j, YS - j).start()
    mine = None
    for k in Z_FAR + (0,):
        total = total_of(along(me_m, k, 0))
        for j in (1, 3, 2):
            y_copy(k, j, j).wait_recv()
            total += y_parts[YS * k + j].astype(jnp.float32)
        if k:
            z_sums[k] = total.astype(jnp.bfloat16)
            z_copy(k, ZS - k).start()
        else:
            mine = total
    for k in Z_NEAR:
        z_copy(k, k).wait_recv()
        mine += z_parts[k].astype(jnp.float32)
    out_ref[0] = mine
    for k in range(1, GROUPS):
        row_copy(k, me_g).wait_send()
    for k in range(ZS):
        for j in range(1, YS):
            y_copy(k, j, j).wait_send()
        if k:
            z_copy(k, k).wait_send()


def give(rows, info):
    return pl.pallas_call(
        give_kernel,
        out_shape=jax.ShapeDtypeStruct((1, TOK, DIM), jnp.float32),
        in_specs=[
            pl.BlockSpec(memory_space=pl.ANY),
            pl.BlockSpec(memory_space=pltpu.SMEM),
        ],
        out_specs=pl.BlockSpec(memory_space=pltpu.VMEM),
        scratch_shapes=[
            pltpu.VMEM((GROUPS * CAP, TOK, DIM), jnp.bfloat16),
            pltpu.VMEM((GROUPS, 2 * CAP, TOK, DIM), jnp.bfloat16),
            pltpu.VMEM((MEMBERS, TOK, DIM), jnp.bfloat16),
            pltpu.VMEM((MEMBERS, TOK, DIM), jnp.bfloat16),
            pltpu.VMEM((ZS, TOK, DIM), jnp.bfloat16),
            pltpu.VMEM((ZS, TOK, DIM), jnp.bfloat16),
            pltpu.SemaphoreType.DMA((GROUPS,)),
            pltpu.SemaphoreType.DMA((GROUPS,)),
            pltpu.SemaphoreType.DMA((MEMBERS,)),
            pltpu.SemaphoreType.DMA((MEMBERS,)),
            pltpu.SemaphoreType.DMA((ZS,)),
            pltpu.SemaphoreType.DMA((ZS,)),
            pltpu.SemaphoreType.DMA,
        ],
        compiler_params=pltpu.CompilerParams(
            collective_id=1, has_side_effects=True, vmem_limit_bytes=60 * 1024 * 1024
        ),
        name="give",
    )(rows, info)


def body(queries, pages, users, page_count, teacher):
    picked, place, info, page_t = fetch(queries, users, pages)
    scores, rows, page_grad = match(place, page_count, teacher, picked, pages, page_t)
    query_grad = give(rows, info)
    return scores, query_grad, page_grad


def solution(mesh):
    both = ("group", "member")
    three, two, one = P(both, None, None), P(both, None), P(both)
    return jax.shard_map(
        body,
        mesh=mesh,
        in_specs=(three, three, two, one, two),
        out_specs=(two, three, three),
        check_vma=False,
    )
```

```python
import functools
import math

import jax
import jax.numpy as jnp
from jax import lax
from jax.experimental import pallas as pl
from jax.experimental.pallas import tpu as pltpu
from jax.sharding import PartitionSpec as P

MESH = pl.DeviceIdType.MESH
CAP = 8
GROUPS = 8
MEMBERS = 32
TOK = 32
ZS, YS = 8, 4
Z_FAR = (4, 3, 5, 2, 6, 1, 7)
Z_NEAR = (1, 7, 2, 6, 3, 5, 4)
Y_FAR = (2, 1, 3)
DIM = 128
CHUNK = 8
LANES = CHUNK * TOK
INV_AT = 32
SCALE = math.log2(math.e) / 0.05
LN2 = math.log(2.0)
TOP, PEAK, MASS, MOMENT, BASE, SLANT = range(6)


def along(me_m, dz, dy):
    return ((me_m // YS + dz) % ZS) * YS + (me_m % YS + dy) % YS


def greet(me_g, me_m):
    barrier = pltpu.get_barrier_semaphore()
    peers = [(me_g, along(me_m, k, 0)) for k in Z_FAR]
    peers += [(me_g, along(me_m, 0, k)) for k in range(1, YS)]
    peers += [((me_g + k) % GROUPS, me_m) for k in range(1, GROUPS)]
    for peer in peers:
        pl.semaphore_signal(barrier, inc=1, device_id=peer, device_id_type=MESH)
    return barrier, len(peers)


def fetch_kernel(
    query_hbm, users_hbm, pages_hbm, picked_hbm, place_hbm, info_hbm, page_t_hbm,
    table, users_ref, place_ref, pages_ref, page_t, asks_out, asks_in, asks_smem, chosen,
    z_send, y_send, q_recv, a_send, a_recv, c_send, c_recv, local_sem, in_sem, out_sem,
):
    me_g = lax.axis_index("group")
    me_m = lax.axis_index("member")
    n_pages = pages_hbm.shape[0]
    barrier, greeted = greet(me_g, me_m)
    users_in = pltpu.make_async_copy(users_hbm, users_ref, local_sem.at[0])
    query_in = pltpu.make_async_copy(query_hbm.at[0], table.at[me_m], local_sem.at[1])
    users_in.start()
    query_in.start()

    def page_in(p):
        return pltpu.make_async_copy(pages_hbm.at[p], pages_ref.at[p], in_sem.at[p])

    def page_out(p):
        return pltpu.make_async_copy(page_t.at[p], page_t_hbm.at[p], out_sem.at[p])

    for p in range(n_pages):
        page_in(p).start()
    users_in.wait()

    total = GROUPS * MEMBERS
    rows = users_ref.shape[0]
    qid = lax.broadcasted_iota(jnp.int32, (total, users_ref.shape[1]), 0)
    hits = [jnp.where(users_ref[p : p + 1, :] == qid, 1.0, 0.0) for p in range(rows)]
    hit = functools.reduce(jnp.maximum, hits)
    count = lax.dot_general(
        jnp.ones((8, users_ref.shape[1]), jnp.bfloat16),
        hit.astype(jnp.bfloat16),
        (((1,), (1,)), ((), ())),
        preferred_element_type=jnp.float32,
    )
    used = jnp.where(count > 0.5, 1.0, 0.0)
    ri = lax.broadcasted_iota(jnp.int32, (total, total), 0)
    ci = lax.broadcasted_iota(jnp.int32, (total, total), 1)
    before = jnp.where((ri < ci) & ((ri >> 5) == (ci >> 5)), 1.0, 0.0).astype(jnp.bfloat16)
    rank = jnp.dot(used.astype(jnp.bfloat16), before, preferred_element_type=jnp.float32)
    lane8 = lax.broadcasted_iota(jnp.int32, (8, total), 1)
    sub8 = lax.broadcasted_iota(jnp.int32, (8, total), 0)
    of_group = (lane8 >> 5) == sub8
    k_id = lax.broadcasted_iota(jnp.int32, (128, total), 0).astype(jnp.float32)
    local_id = (lax.broadcasted_iota(jnp.int32, (128, total), 1) & 31).astype(jnp.float32)
    named = jnp.where((k_id == rank[0:1]) & (used[0:1] > 0.5), local_id, 0.0)
    ids = lax.dot_general(
        jnp.where(of_group, 1.0, 0.0).astype(jnp.bfloat16),
        named.astype(jnp.bfloat16),
        (((1,), (1,)), ((), ())),
        preferred_element_type=jnp.float32,
    )
    inverse = jnp.where(of_group, jnp.where(used > 0.5, rank, float(CAP)), 0.0)
    fold_r = lax.broadcasted_iota(jnp.int32, (total, 128), 0)
    fold_c = lax.broadcasted_iota(jnp.int32, (total, 128), 1)
    fold = jnp.where(fold_c == INV_AT + (fold_r & 31), 1.0, 0.0).astype(jnp.bfloat16)
    spread = jnp.dot(inverse.astype(jnp.bfloat16), fold, preferred_element_type=jnp.float32)
    asks = (ids + spread).astype(jnp.int32)
    for g in range(GROUPS):
        asks_out[g] = asks[g : g + 1, :]
    query_in.wait()

    def remote(src, dst, send, recv, g, m):
        return pltpu.make_async_remote_copy(
            src_ref=src, dst_ref=dst, send_sem=send, recv_sem=recv,
            device_id=(g, m), device_id_type=MESH,
        )

    def z_copy(k, src_m):
        return remote(
            table.at[src_m], table.at[src_m], z_send.at[k], q_recv.at[src_m],
            me_g, along(me_m, k, 0),
        )

    def y_copy(k, j, src_m):
        return remote(
            table.at[src_m], table.at[src_m], y_send.at[YS * k + j], q_recv.at[src_m],
            me_g, along(me_m, 0, j),
        )

    def ask_copy(k, src_g):
        peer = (me_g + k) % GROUPS
        return remote(
            asks_out.at[peer], asks_in.at[src_g], a_send.at[k], a_recv.at[src_g], peer, me_m
        )

    def chosen_copy(k, src_g):
        peer = (me_g + k) % GROUPS
        return remote(
            chosen.at[k], picked_hbm.at[pl.ds(src_g * CAP, CAP)],
            c_send.at[k], c_recv.at[src_g], peer, me_m,
        )

    pl.semaphore_wait(barrier, greeted)
    for k in Z_FAR:
        z_copy(k, me_m).start()
    for j in Y_FAR:
        y_copy(0, j, me_m).start()
    for k in range(1, GROUPS):
        ask_copy(k, me_g).start()
    asks_in[me_g] = asks_out[me_g]
    spot = ((lane8 >> 5) * CAP).astype(jnp.float32) + rank
    for p in range(rows):
        place = jnp.dot(
            spot.astype(jnp.bfloat16), hits[p].astype(jnp.bfloat16),
            preferred_element_type=jnp.float32,
        )
        place_ref[p : p + 1, :] = place[0:1].astype(jnp.int32)
    place_out = pltpu.make_async_copy(place_ref, place_hbm, local_sem.at[2])
    place_out.start()
    for p in range(n_pages):
        page_in(p).wait()
        page_t[p] = pages_ref[p].T
        page_out(p).start()
    for k in Z_NEAR:
        src = along(me_m, k, 0)
        z_copy(k, src).wait_recv()
        for j in Y_FAR:
            y_copy(k, j, src).start()
    for k in range(1, GROUPS):
        ask_copy(k, (me_g + k) % GROUPS).wait_recv()
    to_smem = pltpu.make_async_copy(asks_in, asks_smem, local_sem.at[0])
    to_smem.start()
    info_out = pltpu.make_async_copy(asks_in, info_hbm, local_sem.at[3])
    info_out.start()
    to_smem.wait()
    for k in (0,) + Z_NEAR:
        for j in range(1, YS):
            y_copy(k, j, along(me_m, k, j)).wait_recv()

    for k in (4, 5, 2, 3, 6, 7, 1, 0):
        peer = (me_g + k) % GROUPS
        for n in range(CAP):
            chosen[k, n] = table[asks_smem[peer, 0, n] & (MEMBERS - 1)]
        if k:
            chosen_copy(k, me_g).start()
    own = pltpu.make_async_copy(
        chosen.at[0], picked_hbm.at[pl.ds(me_g * CAP, CAP)], local_sem.at[1]
    )
    own.start()
    for p in range(n_pages):
        page_out(p).wait()
    for k in Z_NEAR:
        z_copy(k, me_m).wait_send()
    for k in (0,) + Z_NEAR:
        for j in range(1, YS):
            y_copy(k, j, along(me_m, k, 0)).wait_send()
    own.wait()
    place_out.wait()
    info_out.wait()
    for k in range(1, GROUPS):
        chosen_copy(k, (me_g + k) % GROUPS).wait_recv()
        ask_copy(k, me_g).wait_send()
        chosen_copy(k, me_g).wait_send()


def fetch(queries, users, pages):
    n_pages, n_tok, _ = pages.shape
    anywhere = pl.BlockSpec(memory_space=pl.ANY)
    return pl.pallas_call(
        fetch_kernel,
        out_shape=(
            jax.ShapeDtypeStruct((GROUPS * CAP, TOK, DIM), jnp.bfloat16),
            jax.ShapeDtypeStruct(users.shape, jnp.int32),
            jax.ShapeDtypeStruct((GROUPS, 1, 128), jnp.int32),
            jax.ShapeDtypeStruct((n_pages, DIM, n_tok), jnp.bfloat16),
        ),
        in_specs=[anywhere] * 3,
        out_specs=[anywhere] * 4,
        scratch_shapes=[
            pltpu.VMEM((MEMBERS, TOK, DIM), jnp.bfloat16),
            pltpu.VMEM(users.shape, jnp.int32),
            pltpu.VMEM(users.shape, jnp.int32),
            pltpu.VMEM(pages.shape, jnp.bfloat16),
            pltpu.VMEM((n_pages, DIM, n_tok), jnp.bfloat16),
            pltpu.VMEM((GROUPS, 1, 128), jnp.int32),
            pltpu.VMEM((GROUPS, 1, 128), jnp.int32),
            pltpu.SMEM((GROUPS, 1, 128), jnp.int32),
            pltpu.VMEM((GROUPS, CAP, TOK, DIM), jnp.bfloat16),
            pltpu.SemaphoreType.DMA((ZS,)),
            pltpu.SemaphoreType.DMA((MEMBERS,)),
            pltpu.SemaphoreType.DMA((MEMBERS,)),
            pltpu.SemaphoreType.DMA((GROUPS,)),
            pltpu.SemaphoreType.DMA((GROUPS,)),
            pltpu.SemaphoreType.DMA((GROUPS,)),
            pltpu.SemaphoreType.DMA((GROUPS,)),
            pltpu.SemaphoreType.DMA((4,)),
            pltpu.SemaphoreType.DMA((n_pages,)),
            pltpu.SemaphoreType.DMA((n_pages,)),
        ],
        compiler_params=pltpu.CompilerParams(
            collective_id=0, has_side_effects=True, vmem_limit_bytes=60 * 1024 * 1024
        ),
        name="fetch",
    )(queries, users, pages)


def split_dot(value, ones):
    high = value.astype(jnp.bfloat16)
    rest = value - high.astype(jnp.float32)
    mid = rest.astype(jnp.bfloat16)
    low = (rest - mid.astype(jnp.float32)).astype(jnp.bfloat16)
    dot = functools.partial(jnp.dot, preferred_element_type=jnp.float32)
    return dot(high, ones) + (dot(mid, ones) + dot(low, ones))


def match_kernel(
    place_hbm, count_hbm, teacher_hbm, picked_hbm, pages_hbm, page_t_hbm,
    scores_ref, rows_ref, grad_hbm,
    chunks, place_ref, count_ref, teacher_ref, picked_ref, scaled, pages_ref, page_t, sims, logit, pending, stats, acc,
    grad_ref, row_acc, score_l, same_slot, in_sem, out_sem, small_sem,
):
    n_pages, n_tok, _ = pages_ref.shape
    per_page = place_ref.shape[1] // CHUNK
    half = n_tok // 2
    quarter = n_tok // 4

    def page_in(p):
        return pltpu.make_async_copy(pages_hbm.at[p], pages_ref.at[p], in_sem.at[p])

    picked_in = pltpu.make_async_copy(picked_hbm, picked_ref, in_sem.at[n_pages])
    turned_in = pltpu.make_async_copy(page_t_hbm, page_t, in_sem.at[n_pages + 1])
    smalls = [
        pltpu.make_async_copy(source, dest, small_sem.at[i])
        for i, (source, dest) in enumerate(
            ((count_hbm, count_ref), (place_hbm, place_ref), (teacher_hbm, teacher_ref))
        )
    ]
    for small in smalls:
        small.start()
    picked_in.start()
    for p in range(n_pages):
        page_in(p).start()
    turned_in.start()

    acc[...] = jnp.zeros_like(acc)
    row_acc[...] = jnp.zeros_like(row_acc)
    score_l[...] = jnp.zeros_like(score_l)
    logit[...] = jnp.zeros_like(logit)
    stats[...] = jnp.zeros_like(stats)
    pending[...] = jnp.zeros_like(pending)
    seg_r = lax.broadcasted_iota(jnp.int32, (LANES, LANES), 0) >> 5
    seg_c = lax.broadcasted_iota(jnp.int32, (LANES, LANES), 1) >> 5
    same_slot[...] = jnp.where(seg_r == seg_c, 1.0, 0.0).astype(jnp.bfloat16)
    slot_of_lane = lax.broadcasted_iota(jnp.int32, (8, LANES), 1) >> 5
    for small in smalls:
        small.wait()

    def list_chunk(n, total):
        p = n // per_page
        alive = (n % per_page) * CHUNK < count_ref[p]

        @pl.when(alive)
        def _():
            chunks[total] = n

        return total + alive.astype(jnp.int32)

    total = lax.fori_loop(0, n_pages * per_page, list_chunk, jnp.int32(0))
    for n in range(3):
        chunks[total + n] = 0
    pairs = (total + 1) // 2
    picked_in.wait()

    def scale_picked(n, carry):
        full = picked_ref[n].astype(jnp.float32) * SCALE
        high = full.astype(jnp.bfloat16)
        scaled[n, :, :DIM] = high
        scaled[n, :, DIM:] = (full - high.astype(jnp.float32)).astype(jnp.bfloat16)
        return carry

    lax.fori_loop(0, picked_ref.shape[0], scale_picked, 0, unroll=8)
    for p in range(n_pages):
        page_in(p).wait()
    turned_in.wait()

    def where_of(n):
        code = chunks[n]
        return code // per_page, code % per_page

    def chosen_of(p, c, source):
        return jnp.concatenate(
            [source[place_ref[p, c * CHUNK + k]] for k in range(CHUNK)], axis=0
        )

    def fold8(value, op):
        parts = [value[8 * i : 8 * i + 8] for i in range(value.shape[0] // 8)]
        while len(parts) > 1:
            parts = [
                op(parts[i], parts[i + 1]) if i + 1 < len(parts) else parts[i]
                for i in range(0, len(parts), 2)
            ]
        return parts[0]

    def tall(value, rows):
        return jnp.concatenate([value] * (rows // 8), axis=0)

    def similar_half(p, chosen, slot, h):
        at = slice(half * h, half * h + half)
        page = pages_ref[p, at, :]
        block = lax.dot_general(
            jnp.concatenate([page, page], axis=1), chosen, (((1,), (1,)), ((), ())),
            preferred_element_type=jnp.float32,
        )
        sims[slot, at, :] = block
        return fold8(block, jnp.maximum)

    def similar(n, slot):
        p, c = where_of(n)
        chosen = chosen_of(p, c, scaled)
        tops = [similar_half(p, chosen, slot, h) for h in range(2)]
        stats[slot, TOP] = jnp.maximum(*tops)

    def weigh_rows(slot, top, start, rows):
        mass = moment = None
        for i in range(rows // 32):
            at = slice(start + 32 * i, start + 32 * i + 32)
            t = sims[slot, at, :] - tall(top, 32)
            e = jnp.exp2(t)
            g = e * t
            logit[slot, at, :] = t
            e, g = fold8(e, jnp.add), fold8(g, jnp.add)
            mass = e if mass is None else mass + e
            moment = g if moment is None else moment + g
        return mass, moment

    def settle(n, slot, begun):
        p, c = where_of(n)
        known = (n < total) & begun
        mass = jnp.broadcast_to(
            jnp.sum(stats[slot, MASS], axis=0, keepdims=True), (8, LANES)
        )
        moment = jnp.broadcast_to(
            jnp.sum(stats[slot, MOMENT], axis=0, keepdims=True), (8, LANES)
        )
        mass = jnp.where(mass > 0.0, mass, 1.0)
        mean = moment / mass
        matched = (stats[slot, PEAK] + mean) * (1.0 / SCALE)
        score = split_dot(matched, same_slot[...])
        taught = jnp.zeros((8, LANES), jnp.float32)
        for k in range(CHUNK):
            taught = jnp.where(slot_of_lane == k, teacher_ref[p, c * CHUNK + k], taught)
        bound = jnp.where(known, count_ref[p] - c * CHUNK, 0)
        live = slot_of_lane < bound
        row = jnp.where(known, p, n_pages)
        score_l[c, pl.ds(row, 1), :] = jnp.where(live, score, 0.0)[0:1]
        part = jnp.where(live, (score - taught) / mass, 0.0)
        slant = part * LN2
        stats[slot, BASE] = part - slant * mean
        stats[slot, SLANT] = slant

    def slope_rows(slot, base, slant, start, rows):
        parts = []
        for i in range(rows // 32):
            at = slice(start + 32 * i, start + 32 * i + 32)
            t = logit[slot, at, :]
            parts.append(
                (jnp.exp2(t) * (tall(base, 32) + tall(slant, 32) * t)).astype(jnp.bfloat16)
            )
        return jnp.concatenate(parts, axis=0)

    def spread_rows(p, chosen, slope, at, query_t):
        acc[p, at, :] += jnp.dot(slope, chosen, preferred_element_type=jnp.float32)
        part = jnp.dot(page_t[p, :, at], slope, preferred_element_type=jnp.float32)
        return part if query_t is None else query_t + part

    def add_rows(n, slot):
        p, c = where_of(n)
        query_part = pending[slot].T
        for k in range(CHUNK):
            row_acc[place_ref[p, c * CHUNK + k]] += query_part[TOK * k : TOK * k + TOK]

    def spread(n, slot):
        p, c = where_of(n)
        chosen = chosen_of(p, c, picked_ref)
        base, slant = stats[slot, BASE], stats[slot, SLANT]
        query_t = None
        for b in range(4):
            at = slice(quarter * b, quarter * b + quarter)
            slope = slope_rows(slot, base, slant, quarter * b, quarter)
            query_t = spread_rows(p, chosen, slope, at, query_t)
        pending[slot] = query_t

    def turn(old, now, new, slot):
        p_old, c_old = where_of(old)
        p_new, c_new = where_of(new)
        chosen_old = chosen_of(p_old, c_old, picked_ref)
        chosen_new = chosen_of(p_new, c_new, scaled)
        base, slant = stats[slot, BASE], stats[slot, SLANT]
        top = jnp.broadcast_to(
            jnp.max(stats[slot, TOP], axis=0, keepdims=True), (8, LANES)
        )
        stats[slot, PEAK] = top
        query_t = mass = moment = None
        tops = []
        for h in range(2):
            for b in (2 * h, 2 * h + 1):
                at = slice(quarter * b, quarter * b + quarter)
                slope = slope_rows(slot, base, slant, quarter * b, quarter)
                query_t = spread_rows(p_old, chosen_old, slope, at, query_t)
                e, g = weigh_rows(slot, top, quarter * b, quarter)
                mass = e if mass is None else mass + e
                moment = g if moment is None else moment + g
            tops.append(similar_half(p_new, chosen_new, slot, h))
        stats[slot, TOP] = jnp.maximum(*tops)
        stats[slot, MASS] = mass
        stats[slot, MOMENT] = moment
        pending[slot] = query_t

    similar(0, 0)
    similar(1, 1)

    def step(i, carry):
        n = 2 * i
        old = jnp.maximum(n - 2, 0)

        settle(old + 1, 1, i > 0)
        add_rows(jnp.maximum(n - 3, 0), 1)
        turn(old, n, n + 2, 0)
        settle(n, 0, True)
        add_rows(old, 0)
        turn(old + 1, n + 1, n + 3, 1)
        return carry

    lax.fori_loop(0, pairs, step, 0)

    def page_out(p):
        return pltpu.make_async_copy(grad_ref.at[p], grad_hbm.at[p], out_sem.at[p])

    for p in range(n_pages - 2):
        grad_ref[p] = acc[p].astype(jnp.bfloat16)
        page_out(p).start()
    last = 2 * pairs - 1
    settle(last, 1, True)
    add_rows(jnp.maximum(last - 2, 0), 1)
    spread(last - 1, 0)
    spread(last, 1)
    add_rows(last - 1, 0)
    add_rows(last, 1)
    for p in range(n_pages - 2, n_pages):
        grad_ref[p] = acc[p].astype(jnp.bfloat16)
        page_out(p).start()
    col = lax.broadcasted_iota(jnp.int32, (LANES, 128), 1)
    row = lax.broadcasted_iota(jnp.int32, (LANES, 128), 0)
    out = jnp.zeros((8, 128), jnp.float32)
    for c in range(per_page):
        take = jnp.where(row == (col - c * CHUNK) * TOK, 1.0, 0.0)
        out += split_dot(score_l[c], take.astype(jnp.bfloat16))
    scores_ref[...] = out[: scores_ref.shape[0], : scores_ref.shape[1]]
    rows_ref[...] = row_acc[...].astype(jnp.bfloat16)
    for p in range(n_pages):
        page_out(p).wait()


def match(place, page_count, teacher, picked, pages, page_t):
    n_pages, n_tok, _ = pages.shape
    per_page = teacher.shape[1] // CHUNK
    vmem = pl.BlockSpec(memory_space=pltpu.VMEM)
    anywhere = pl.BlockSpec(memory_space=pl.ANY)
    return pl.pallas_call(
        match_kernel,
        out_shape=(
            jax.ShapeDtypeStruct(teacher.shape, jnp.float32),
            jax.ShapeDtypeStruct(picked.shape, jnp.bfloat16),
            jax.ShapeDtypeStruct(pages.shape, jnp.bfloat16),
        ),
        in_specs=[anywhere] * 6,
        out_specs=[vmem, vmem, anywhere],
        scratch_shapes=[
            pltpu.SMEM((n_pages * per_page + 3,), jnp.int32),
            pltpu.SMEM(place.shape, jnp.int32),
            pltpu.SMEM(page_count.shape, jnp.int32),
            pltpu.SMEM(teacher.shape, jnp.float32),
            pltpu.VMEM(picked.shape, jnp.bfloat16),
            pltpu.VMEM((GROUPS * CAP, TOK, 2 * DIM), jnp.bfloat16),
            pltpu.VMEM(pages.shape, jnp.bfloat16),
            pltpu.VMEM((n_pages, DIM, n_tok), jnp.bfloat16),
            pltpu.VMEM((2, n_tok, LANES), jnp.float32),
            pltpu.VMEM((2, n_tok, LANES), jnp.float32),
            pltpu.VMEM((2, DIM, LANES), jnp.float32),
            pltpu.VMEM((2, 6, 8, LANES), jnp.float32),
            pltpu.VMEM((n_pages, n_tok, DIM), jnp.float32),
            pltpu.VMEM(pages.shape, jnp.bfloat16),
            pltpu.VMEM(picked.shape, jnp.float32),
            pltpu.VMEM((per_page, 8, LANES), jnp.float32),
            pltpu.VMEM((LANES, LANES), jnp.bfloat16),
            pltpu.SemaphoreType.DMA((n_pages + 2,)),
            pltpu.SemaphoreType.DMA((n_pages,)),
            pltpu.SemaphoreType.DMA((3,)),
        ],
        compiler_params=pltpu.CompilerParams(vmem_limit_bytes=60 * 1024 * 1024),
        name="match",
    )(place, page_count, teacher, picked, pages, page_t)


def give_kernel(
    rows_hbm, info_hbm, out_ref,
    rows_ref, info_ref, landed, table, y_parts, z_sums, z_parts,
    r_send, r_recv, y_send, y_recv, z_send, z_recv, local_sem,
):
    me_g = lax.axis_index("group")
    me_m = lax.axis_index("member")
    barrier, greeted = greet(me_g, me_m)
    rows_in = pltpu.make_async_copy(rows_hbm, rows_ref, local_sem.at[0])
    info_in = pltpu.make_async_copy(info_hbm, info_ref, local_sem.at[1])
    rows_in.start()
    info_in.start()
    for s in range(GROUPS):
        for spare in range(CAP, 2 * CAP):
            landed[s, spare] = jnp.zeros((TOK, DIM), jnp.bfloat16)
    rows_in.wait()
    info_in.wait()
    for n in range(CAP):
        landed[me_g, n] = rows_ref[me_g * CAP + n]
    pl.semaphore_wait(barrier, greeted)

    def remote(src, dst, send, recv, g, m):
        return pltpu.make_async_remote_copy(
            src_ref=src, dst_ref=dst, send_sem=send, recv_sem=recv,
            device_id=(g, m), device_id_type=MESH,
        )

    def row_copy(k, src_g):
        peer = (me_g + k) % GROUPS
        return remote(
            rows_ref.at[pl.ds(peer * CAP, CAP)], landed.at[src_g, pl.ds(0, CAP)],
            r_send.at[k], r_recv.at[src_g], peer, me_m,
        )

    def y_copy(k, j, slot):
        return remote(
            table.at[YS * k + j], y_parts.at[YS * k + slot],
            y_send.at[YS * k + j], y_recv.at[YS * k + slot], me_g, along(me_m, 0, j),
        )

    def z_copy(k, slot):
        return remote(
            z_sums.at[k], z_parts.at[slot], z_send.at[k], z_recv.at[slot],
            me_g, along(me_m, k, 0),
        )

    for k in (4, 5, 2, 3, 6, 7, 1):
        row_copy(k, me_g).start()
    for k in range(1, GROUPS):
        row_copy(k, (me_g + k) % GROUPS).wait_recv()

    def total_of(owner):
        total = jnp.zeros((TOK, DIM), jnp.float32)
        for s in range(GROUPS):
            total += landed[s, info_ref[s, 0, INV_AT + owner] & (2 * CAP - 1)].astype(
                jnp.float32
            )
        return total

    for k in Z_FAR + (0,):
        for j in Y_FAR:
            table[YS * k + j] = total_of(along(me_m, k, j)).astype(jnp.bfloat16)
            y_copy(k, j, YS - j).start()
    mine = None
    for k in Z_FAR + (0,):
        total = total_of(along(me_m, k, 0))
        for j in (1, 3, 2):
            y_copy(k, j, j).wait_recv()
            total += y_parts[YS * k + j].astype(jnp.float32)
        if k:
            z_sums[k] = total.astype(jnp.bfloat16)
            z_copy(k, ZS - k).start()
        else:
            mine = total
    for k in Z_NEAR:
        z_copy(k, k).wait_recv()
        mine += z_parts[k].astype(jnp.float32)
    out_ref[0] = mine
    for k in range(1, GROUPS):
        row_copy(k, me_g).wait_send()
    for k in range(ZS):
        for j in range(1, YS):
            y_copy(k, j, j).wait_send()
        if k:
            z_copy(k, k).wait_send()


def give(rows, info):
    return pl.pallas_call(
        give_kernel,
        out_shape=jax.ShapeDtypeStruct((1, TOK, DIM), jnp.float32),
        in_specs=[
            pl.BlockSpec(memory_space=pl.ANY),
            pl.BlockSpec(memory_space=pl.ANY),
        ],
        out_specs=pl.BlockSpec(memory_space=pltpu.VMEM),
        scratch_shapes=[
            pltpu.VMEM((GROUPS * CAP, TOK, DIM), jnp.bfloat16),
            pltpu.SMEM(info.shape, jnp.int32),
            pltpu.VMEM((GROUPS, 2 * CAP, TOK, DIM), jnp.bfloat16),
            pltpu.VMEM((MEMBERS, TOK, DIM), jnp.bfloat16),
            pltpu.VMEM((MEMBERS, TOK, DIM), jnp.bfloat16),
            pltpu.VMEM((ZS, TOK, DIM), jnp.bfloat16),
            pltpu.VMEM((ZS, TOK, DIM), jnp.bfloat16),
            pltpu.SemaphoreType.DMA((GROUPS,)),
            pltpu.SemaphoreType.DMA((GROUPS,)),
            pltpu.SemaphoreType.DMA((MEMBERS,)),
            pltpu.SemaphoreType.DMA((MEMBERS,)),
            pltpu.SemaphoreType.DMA((ZS,)),
            pltpu.SemaphoreType.DMA((ZS,)),
            pltpu.SemaphoreType.DMA((2,)),
        ],
        compiler_params=pltpu.CompilerParams(
            collective_id=1, has_side_effects=True, vmem_limit_bytes=60 * 1024 * 1024
        ),
        name="give",
    )(rows, info)


def body(queries, pages, users, page_count, teacher):
    picked, place, info, page_t = fetch(queries, users, pages)
    scores, rows, page_grad = match(place, page_count, teacher, picked, pages, page_t)
    query_grad = give(rows, info)
    return scores, query_grad, page_grad


def solution(mesh):
    both = ("group", "member")
    three, two, one = P(both, None, None), P(both, None), P(both)
    return jax.shard_map(
        body,
        mesh=mesh,
        in_specs=(three, three, two, one, two),
        out_specs=(two, three, three),
        check_vma=False,
    )
```

```python
import functools
import math

import jax
import jax.numpy as jnp
from jax import lax
from jax.experimental import pallas as pl
from jax.experimental.pallas import tpu as pltpu
from jax.sharding import PartitionSpec as P

MESH = pl.DeviceIdType.MESH
CAP = 8
GROUPS = 8
MEMBERS = 32
TOK = 32
HALF = TOK // 2
ZS, YS = 8, 4
Z_FAR = (4, 3, 5, 2, 6, 1, 7)
Z_NEAR = (1, 7, 2, 6, 3, 5, 4)
Y_FAR = (2, 1, 3)
DIM = 128
CHUNK = 8
LANES = CHUNK * TOK
INV_AT = 32
SCALE = math.log2(math.e) / 0.05
LN2 = math.log(2.0)
TOP, PEAK, MASS, MOMENT, BASE, SLANT = range(6)


def along(me_m, dz, dy):
    return ((me_m // YS + dz) % ZS) * YS + (me_m % YS + dy) % YS


def greet(me_g, me_m):
    barrier = pltpu.get_barrier_semaphore()
    peers = [(me_g, along(me_m, k, 0)) for k in Z_FAR]
    peers += [(me_g, along(me_m, 0, k)) for k in range(1, YS)]
    peers += [((me_g + k) % GROUPS, me_m) for k in range(1, GROUPS)]
    for peer in peers:
        pl.semaphore_signal(barrier, inc=1, device_id=peer, device_id_type=MESH)
    return barrier, len(peers)


def fetch_kernel(
    query_hbm, users_hbm, pages_hbm, picked_hbm, place_hbm, info_hbm, page_t_hbm,
    table, users_ref, place_ref, pages_ref, page_t, asks_out, asks_in, asks_smem, chosen,
    z_send, y_send, q_recv, a_send, a_recv, c_send, c_recv, local_sem, in_sem, out_sem,
):
    me_g = lax.axis_index("group")
    me_m = lax.axis_index("member")
    n_pages = pages_hbm.shape[0]
    barrier, greeted = greet(me_g, me_m)
    users_in = pltpu.make_async_copy(users_hbm, users_ref, local_sem.at[0])
    query_in = pltpu.make_async_copy(query_hbm.at[0], table.at[me_m], local_sem.at[1])
    users_in.start()
    query_in.start()

    def page_in(p):
        return pltpu.make_async_copy(pages_hbm.at[p], pages_ref.at[p], in_sem.at[p])

    def page_out(p):
        return pltpu.make_async_copy(page_t.at[p], page_t_hbm.at[p], out_sem.at[p])

    for p in range(n_pages):
        page_in(p).start()
    users_in.wait()

    total = GROUPS * MEMBERS
    rows = users_ref.shape[0]
    qid = lax.broadcasted_iota(jnp.int32, (total, users_ref.shape[1]), 0)
    hits = [jnp.where(users_ref[p : p + 1, :] == qid, 1.0, 0.0) for p in range(rows)]
    hit = functools.reduce(jnp.maximum, hits)
    count = lax.dot_general(
        jnp.ones((8, users_ref.shape[1]), jnp.bfloat16),
        hit.astype(jnp.bfloat16),
        (((1,), (1,)), ((), ())),
        preferred_element_type=jnp.float32,
    )
    used = jnp.where(count > 0.5, 1.0, 0.0)
    ri = lax.broadcasted_iota(jnp.int32, (total, total), 0)
    ci = lax.broadcasted_iota(jnp.int32, (total, total), 1)
    before = jnp.where((ri < ci) & ((ri >> 5) == (ci >> 5)), 1.0, 0.0).astype(jnp.bfloat16)
    rank = jnp.dot(used.astype(jnp.bfloat16), before, preferred_element_type=jnp.float32)
    lane8 = lax.broadcasted_iota(jnp.int32, (8, total), 1)
    sub8 = lax.broadcasted_iota(jnp.int32, (8, total), 0)
    of_group = (lane8 >> 5) == sub8
    k_id = lax.broadcasted_iota(jnp.int32, (128, total), 0).astype(jnp.float32)
    local_id = (lax.broadcasted_iota(jnp.int32, (128, total), 1) & 31).astype(jnp.float32)
    named = jnp.where((k_id == rank[0:1]) & (used[0:1] > 0.5), local_id, 0.0)
    ids = lax.dot_general(
        jnp.where(of_group, 1.0, 0.0).astype(jnp.bfloat16),
        named.astype(jnp.bfloat16),
        (((1,), (1,)), ((), ())),
        preferred_element_type=jnp.float32,
    )
    inverse = jnp.where(of_group, jnp.where(used > 0.5, rank, float(CAP)), 0.0)
    fold_r = lax.broadcasted_iota(jnp.int32, (total, 128), 0)
    fold_c = lax.broadcasted_iota(jnp.int32, (total, 128), 1)
    fold = jnp.where(fold_c == INV_AT + (fold_r & 31), 1.0, 0.0).astype(jnp.bfloat16)
    spread = jnp.dot(inverse.astype(jnp.bfloat16), fold, preferred_element_type=jnp.float32)
    asks = (ids + spread).astype(jnp.int32)
    for g in range(GROUPS):
        asks_out[g] = asks[g : g + 1, :]
    query_in.wait()

    def remote(src, dst, send, recv, g, m):
        return pltpu.make_async_remote_copy(
            src_ref=src, dst_ref=dst, send_sem=send, recv_sem=recv,
            device_id=(g, m), device_id_type=MESH,
        )

    def z_copy(k, src_m):
        return remote(
            table.at[src_m], table.at[src_m], z_send.at[k], q_recv.at[src_m],
            me_g, along(me_m, k, 0),
        )

    def y_copy(k, j, src_m):
        return remote(
            table.at[src_m], table.at[src_m], y_send.at[YS * k + j], q_recv.at[src_m],
            me_g, along(me_m, 0, j),
        )

    def ask_copy(k, src_g):
        peer = (me_g + k) % GROUPS
        return remote(
            asks_out.at[peer], asks_in.at[src_g], a_send.at[k], a_recv.at[src_g], peer, me_m
        )

    def chosen_copy(k, src_g):
        peer = (me_g + k) % GROUPS
        return remote(
            chosen.at[k], picked_hbm.at[pl.ds(src_g * CAP, CAP)],
            c_send.at[k], c_recv.at[src_g], peer, me_m,
        )

    pl.semaphore_wait(barrier, greeted)
    for k in Z_FAR:
        z_copy(k, me_m).start()
    for j in Y_FAR:
        y_copy(0, j, me_m).start()
    for k in range(1, GROUPS):
        ask_copy(k, me_g).start()
    asks_in[me_g] = asks_out[me_g]
    spot = ((lane8 >> 5) * CAP).astype(jnp.float32) + rank
    for p in range(rows):
        place = jnp.dot(
            spot.astype(jnp.bfloat16), hits[p].astype(jnp.bfloat16),
            preferred_element_type=jnp.float32,
        )
        place_ref[p : p + 1, :] = place[0:1].astype(jnp.int32)
    place_out = pltpu.make_async_copy(place_ref, place_hbm, local_sem.at[2])
    place_out.start()
    for p in range(n_pages):
        page_in(p).wait()
        page_t[p] = pages_ref[p].T
        page_out(p).start()
    for k in Z_NEAR:
        src = along(me_m, k, 0)
        z_copy(k, src).wait_recv()
        for j in Y_FAR:
            y_copy(k, j, src).start()
    for k in range(1, GROUPS):
        ask_copy(k, (me_g + k) % GROUPS).wait_recv()
    to_smem = pltpu.make_async_copy(asks_in, asks_smem, local_sem.at[0])
    to_smem.start()
    info_out = pltpu.make_async_copy(asks_in, info_hbm, local_sem.at[3])
    info_out.start()
    to_smem.wait()
    for k in (0,) + Z_NEAR:
        for j in range(1, YS):
            y_copy(k, j, along(me_m, k, j)).wait_recv()

    for k in (4, 5, 2, 3, 6, 7, 1, 0):
        peer = (me_g + k) % GROUPS
        for n in range(CAP):
            chosen[k, n] = table[asks_smem[peer, 0, n] & (MEMBERS - 1)]
        if k:
            chosen_copy(k, me_g).start()
    own = pltpu.make_async_copy(
        chosen.at[0], picked_hbm.at[pl.ds(me_g * CAP, CAP)], local_sem.at[1]
    )
    own.start()
    for p in range(n_pages):
        page_out(p).wait()
    for k in Z_NEAR:
        z_copy(k, me_m).wait_send()
    for k in (0,) + Z_NEAR:
        for j in range(1, YS):
            y_copy(k, j, along(me_m, k, 0)).wait_send()
    own.wait()
    place_out.wait()
    info_out.wait()
    for k in range(1, GROUPS):
        chosen_copy(k, (me_g + k) % GROUPS).wait_recv()
        ask_copy(k, me_g).wait_send()
        chosen_copy(k, me_g).wait_send()


def fetch(queries, users, pages):
    n_pages, n_tok, _ = pages.shape
    anywhere = pl.BlockSpec(memory_space=pl.ANY)
    return pl.pallas_call(
        fetch_kernel,
        out_shape=(
            jax.ShapeDtypeStruct((GROUPS * CAP, TOK, DIM), jnp.bfloat16),
            jax.ShapeDtypeStruct(users.shape, jnp.int32),
            jax.ShapeDtypeStruct((GROUPS, 1, 128), jnp.int32),
            jax.ShapeDtypeStruct((n_pages, DIM, n_tok), jnp.bfloat16),
        ),
        in_specs=[anywhere] * 3,
        out_specs=[anywhere] * 4,
        scratch_shapes=[
            pltpu.VMEM((MEMBERS, TOK, DIM), jnp.bfloat16),
            pltpu.VMEM(users.shape, jnp.int32),
            pltpu.VMEM(users.shape, jnp.int32),
            pltpu.VMEM(pages.shape, jnp.bfloat16),
            pltpu.VMEM((n_pages, DIM, n_tok), jnp.bfloat16),
            pltpu.VMEM((GROUPS, 1, 128), jnp.int32),
            pltpu.VMEM((GROUPS, 1, 128), jnp.int32),
            pltpu.SMEM((GROUPS, 1, 128), jnp.int32),
            pltpu.VMEM((GROUPS, CAP, TOK, DIM), jnp.bfloat16),
            pltpu.SemaphoreType.DMA((ZS,)),
            pltpu.SemaphoreType.DMA((MEMBERS,)),
            pltpu.SemaphoreType.DMA((MEMBERS,)),
            pltpu.SemaphoreType.DMA((GROUPS,)),
            pltpu.SemaphoreType.DMA((GROUPS,)),
            pltpu.SemaphoreType.DMA((GROUPS,)),
            pltpu.SemaphoreType.DMA((GROUPS,)),
            pltpu.SemaphoreType.DMA((4,)),
            pltpu.SemaphoreType.DMA((n_pages,)),
            pltpu.SemaphoreType.DMA((n_pages,)),
        ],
        compiler_params=pltpu.CompilerParams(
            collective_id=0, has_side_effects=True, vmem_limit_bytes=60 * 1024 * 1024
        ),
        name="fetch",
    )(queries, users, pages)


def split_dot(value, ones):
    high = value.astype(jnp.bfloat16)
    rest = value - high.astype(jnp.float32)
    mid = rest.astype(jnp.bfloat16)
    low = (rest - mid.astype(jnp.float32)).astype(jnp.bfloat16)
    dot = functools.partial(jnp.dot, preferred_element_type=jnp.float32)
    return dot(high, ones) + (dot(mid, ones) + dot(low, ones))


def match_kernel(
    place_hbm, count_hbm, teacher_hbm, picked_hbm, pages_hbm, page_t_hbm,
    scores_hbm, rows_hbm, grad_hbm,
    chunks, place_ref, count_ref, teacher_ref, picked_ref, scaled, pages_ref, page_t, sims, logit, pending, stats, acc,
    grad_ref, row_acc, score_l, same_slot, scores_ref, rows_ref, in_sem, out_sem, small_sem,
):
    n_pages, n_tok, _ = pages_ref.shape
    per_page = place_ref.shape[1] // CHUNK
    half = n_tok // 2
    quarter = n_tok // 4

    def page_in(p):
        return pltpu.make_async_copy(pages_hbm.at[p], pages_ref.at[p], in_sem.at[p])

    picked_in = pltpu.make_async_copy(picked_hbm, picked_ref, in_sem.at[n_pages])
    turned_in = pltpu.make_async_copy(page_t_hbm, page_t, in_sem.at[n_pages + 1])
    smalls = [
        pltpu.make_async_copy(source, dest, small_sem.at[i])
        for i, (source, dest) in enumerate(
            ((count_hbm, count_ref), (place_hbm, place_ref), (teacher_hbm, teacher_ref))
        )
    ]
    for small in smalls:
        small.start()
    picked_in.start()
    for p in range(n_pages):
        page_in(p).start()
    turned_in.start()

    acc[...] = jnp.zeros_like(acc)
    row_acc[...] = jnp.zeros_like(row_acc)
    score_l[...] = jnp.zeros_like(score_l)
    logit[...] = jnp.zeros_like(logit)
    stats[...] = jnp.zeros_like(stats)
    pending[...] = jnp.zeros_like(pending)
    seg_r = lax.broadcasted_iota(jnp.int32, (LANES, LANES), 0) >> 5
    seg_c = lax.broadcasted_iota(jnp.int32, (LANES, LANES), 1) >> 5
    same_slot[...] = jnp.where(seg_r == seg_c, 1.0, 0.0).astype(jnp.bfloat16)
    slot_of_lane = lax.broadcasted_iota(jnp.int32, (8, LANES), 1) >> 5
    for small in smalls:
        small.wait()

    def list_chunk(n, total):
        p = n // per_page
        alive = (n % per_page) * CHUNK < count_ref[p]

        @pl.when(alive)
        def _():
            chunks[total] = n

        return total + alive.astype(jnp.int32)

    total = lax.fori_loop(0, n_pages * per_page, list_chunk, jnp.int32(0))
    for n in range(3):
        chunks[total + n] = 0
    pairs = (total + 1) // 2
    picked_in.wait()

    def scale_picked(n, carry):
        full = picked_ref[n].astype(jnp.float32) * SCALE
        high = full.astype(jnp.bfloat16)
        scaled[n, :, :DIM] = high
        scaled[n, :, DIM:] = (full - high.astype(jnp.float32)).astype(jnp.bfloat16)
        return carry

    lax.fori_loop(0, picked_ref.shape[0], scale_picked, 0, unroll=8)
    for p in range(2):
        page_in(p).wait()

    def where_of(n):
        code = chunks[n]
        return code // per_page, code % per_page

    def chosen_of(p, c, source):
        return jnp.concatenate(
            [source[place_ref[p, c * CHUNK + k]] for k in range(CHUNK)], axis=0
        )

    def fold8(value, op):
        parts = [value[8 * i : 8 * i + 8] for i in range(value.shape[0] // 8)]
        while len(parts) > 1:
            parts = [
                op(parts[i], parts[i + 1]) if i + 1 < len(parts) else parts[i]
                for i in range(0, len(parts), 2)
            ]
        return parts[0]

    def tall(value, rows):
        return jnp.concatenate([value] * (rows // 8), axis=0)

    def similar_half(p, chosen, slot, h):
        at = slice(half * h, half * h + half)
        page = pages_ref[p, at, :]
        block = lax.dot_general(
            jnp.concatenate([page, page], axis=1), chosen, (((1,), (1,)), ((), ())),
            preferred_element_type=jnp.float32,
        )
        sims[slot, at, :] = block
        return fold8(block, jnp.maximum)

    def similar(n, slot):
        p, c = where_of(n)
        chosen = chosen_of(p, c, scaled)
        tops = [similar_half(p, chosen, slot, h) for h in range(2)]
        stats[slot, TOP] = jnp.maximum(*tops)

    def weigh_rows(slot, top, start, rows):
        mass = moment = None
        for i in range(rows // 32):
            at = slice(start + 32 * i, start + 32 * i + 32)
            t = sims[slot, at, :] - tall(top, 32)
            e = jnp.exp2(t)
            g = e * t
            logit[slot, at, :] = t
            e, g = fold8(e, jnp.add), fold8(g, jnp.add)
            mass = e if mass is None else mass + e
            moment = g if moment is None else moment + g
        return mass, moment

    def settle(n, slot, begun):
        p, c = where_of(n)
        known = (n < total) & begun
        mass = jnp.broadcast_to(
            jnp.sum(stats[slot, MASS], axis=0, keepdims=True), (8, LANES)
        )
        moment = jnp.broadcast_to(
            jnp.sum(stats[slot, MOMENT], axis=0, keepdims=True), (8, LANES)
        )
        mass = jnp.where(mass > 0.0, mass, 1.0)
        mean = moment / mass
        matched = (stats[slot, PEAK] + mean) * (1.0 / SCALE)
        score = split_dot(matched, same_slot[...])
        taught = jnp.zeros((8, LANES), jnp.float32)
        for k in range(CHUNK):
            taught = jnp.where(slot_of_lane == k, teacher_ref[p, c * CHUNK + k], taught)
        bound = jnp.where(known, count_ref[p] - c * CHUNK, 0)
        live = slot_of_lane < bound
        row = jnp.where(known, p, n_pages)
        score_l[c, pl.ds(row, 1), :] = jnp.where(live, score, 0.0)[0:1]
        part = jnp.where(live, (score - taught) / mass, 0.0)
        slant = part * LN2
        stats[slot, BASE] = part - slant * mean
        stats[slot, SLANT] = slant

    def slope_rows(slot, base, slant, start, rows):
        parts = []
        for i in range(rows // 32):
            at = slice(start + 32 * i, start + 32 * i + 32)
            t = logit[slot, at, :]
            parts.append(
                (jnp.exp2(t) * (tall(base, 32) + tall(slant, 32) * t)).astype(jnp.bfloat16)
            )
        return jnp.concatenate(parts, axis=0)

    def spread_rows(p, chosen, slope, at, query_t):
        acc[p, at, :] += jnp.dot(slope, chosen, preferred_element_type=jnp.float32)
        part = jnp.dot(page_t[p, :, at], slope, preferred_element_type=jnp.float32)
        return part if query_t is None else query_t + part

    def add_rows(n, slot):
        p, c = where_of(n)
        query_part = pending[slot].T
        for k in range(CHUNK):
            row_acc[place_ref[p, c * CHUNK + k]] += query_part[TOK * k : TOK * k + TOK]

    def spread(n, slot):
        p, c = where_of(n)
        chosen = chosen_of(p, c, picked_ref)
        base, slant = stats[slot, BASE], stats[slot, SLANT]
        query_t = None
        for b in range(4):
            at = slice(quarter * b, quarter * b + quarter)
            slope = slope_rows(slot, base, slant, quarter * b, quarter)
            query_t = spread_rows(p, chosen, slope, at, query_t)
        pending[slot] = query_t

    def turn(old, now, new, slot):
        p_old, c_old = where_of(old)
        p_new, c_new = where_of(new)
        chosen_old = chosen_of(p_old, c_old, picked_ref)
        chosen_new = chosen_of(p_new, c_new, scaled)
        base, slant = stats[slot, BASE], stats[slot, SLANT]
        top = jnp.broadcast_to(
            jnp.max(stats[slot, TOP], axis=0, keepdims=True), (8, LANES)
        )
        stats[slot, PEAK] = top
        query_t = mass = moment = None
        tops = []
        for h in range(2):
            for b in (2 * h, 2 * h + 1):
                at = slice(quarter * b, quarter * b + quarter)
                slope = slope_rows(slot, base, slant, quarter * b, quarter)
                query_t = spread_rows(p_old, chosen_old, slope, at, query_t)
                e, g = weigh_rows(slot, top, quarter * b, quarter)
                mass = e if mass is None else mass + e
                moment = g if moment is None else moment + g
            tops.append(similar_half(p_new, chosen_new, slot, h))
        stats[slot, TOP] = jnp.maximum(*tops)
        stats[slot, MASS] = mass
        stats[slot, MOMENT] = moment
        pending[slot] = query_t

    similar(0, 0)
    similar(1, 1)
    for p in range(2, n_pages):
        page_in(p).wait()
    turned_in.wait()

    def step(i, carry):
        n = 2 * i
        old = jnp.maximum(n - 2, 0)

        settle(old + 1, 1, i > 0)
        add_rows(jnp.maximum(n - 3, 0), 1)
        turn(old, n, n + 2, 0)
        settle(n, 0, True)
        add_rows(old, 0)
        turn(old + 1, n + 1, n + 3, 1)
        return carry

    lax.fori_loop(0, pairs, step, 0)

    def page_out(p):
        return pltpu.make_async_copy(grad_ref.at[p], grad_hbm.at[p], out_sem.at[p])

    for p in range(n_pages - 2):
        grad_ref[p] = acc[p].astype(jnp.bfloat16)
        page_out(p).start()
    last = 2 * pairs - 1
    settle(last, 1, True)
    add_rows(jnp.maximum(last - 2, 0), 1)
    spread(last - 1, 0)
    spread(last, 1)
    for p in range(n_pages - 2, n_pages):
        grad_ref[p] = acc[p].astype(jnp.bfloat16)
        page_out(p).start()
    add_rows(last - 1, 0)
    add_rows(last, 1)
    rows_ref[...] = row_acc[...].astype(jnp.bfloat16)
    rows_out = pltpu.make_async_copy(rows_ref, rows_hbm, small_sem.at[0])
    rows_out.start()
    col = lax.broadcasted_iota(jnp.int32, (LANES, 128), 1)
    row = lax.broadcasted_iota(jnp.int32, (LANES, 128), 0)
    out = jnp.zeros((8, 128), jnp.float32)
    for c in range(per_page):
        take = jnp.where(row == (col - c * CHUNK) * TOK, 1.0, 0.0)
        out += split_dot(score_l[c], take.astype(jnp.bfloat16))
    scores_ref[...] = out[: scores_ref.shape[0], : scores_ref.shape[1]]
    scores_out = pltpu.make_async_copy(scores_ref, scores_hbm, small_sem.at[1])
    scores_out.start()
    rows_out.wait()
    scores_out.wait()
    for p in range(n_pages):
        page_out(p).wait()


def match(place, page_count, teacher, picked, pages, page_t):
    n_pages, n_tok, _ = pages.shape
    per_page = teacher.shape[1] // CHUNK
    anywhere = pl.BlockSpec(memory_space=pl.ANY)
    return pl.pallas_call(
        match_kernel,
        out_shape=(
            jax.ShapeDtypeStruct(teacher.shape, jnp.float32),
            jax.ShapeDtypeStruct(picked.shape, jnp.bfloat16),
            jax.ShapeDtypeStruct(pages.shape, jnp.bfloat16),
        ),
        in_specs=[anywhere] * 6,
        out_specs=[anywhere] * 3,
        scratch_shapes=[
            pltpu.SMEM((n_pages * per_page + 3,), jnp.int32),
            pltpu.SMEM(place.shape, jnp.int32),
            pltpu.SMEM(page_count.shape, jnp.int32),
            pltpu.SMEM(teacher.shape, jnp.float32),
            pltpu.VMEM(picked.shape, jnp.bfloat16),
            pltpu.VMEM((GROUPS * CAP, TOK, 2 * DIM), jnp.bfloat16),
            pltpu.VMEM(pages.shape, jnp.bfloat16),
            pltpu.VMEM((n_pages, DIM, n_tok), jnp.bfloat16),
            pltpu.VMEM((2, n_tok, LANES), jnp.float32),
            pltpu.VMEM((2, n_tok, LANES), jnp.float32),
            pltpu.VMEM((2, DIM, LANES), jnp.float32),
            pltpu.VMEM((2, 6, 8, LANES), jnp.float32),
            pltpu.VMEM((n_pages, n_tok, DIM), jnp.float32),
            pltpu.VMEM(pages.shape, jnp.bfloat16),
            pltpu.VMEM(picked.shape, jnp.float32),
            pltpu.VMEM((per_page, 8, LANES), jnp.float32),
            pltpu.VMEM((LANES, LANES), jnp.bfloat16),
            pltpu.VMEM(teacher.shape, jnp.float32),
            pltpu.VMEM(picked.shape, jnp.bfloat16),
            pltpu.SemaphoreType.DMA((n_pages + 2,)),
            pltpu.SemaphoreType.DMA((n_pages,)),
            pltpu.SemaphoreType.DMA((3,)),
        ],
        compiler_params=pltpu.CompilerParams(vmem_limit_bytes=60 * 1024 * 1024),
        name="match",
    )(place, page_count, teacher, picked, pages, page_t)


def give_kernel(
    rows_hbm, info_hbm, out_ref,
    rows_ref, info_ref, landed_a, landed_b, table, y_parts, z_sums, z_parts,
    r_send, r_recv, y_send, y_recv, z_send, z_recv, local_sem,
):
    me_g = lax.axis_index("group")
    me_m = lax.axis_index("member")
    barrier, greeted = greet(me_g, me_m)
    rows_in = pltpu.make_async_copy(rows_hbm, rows_ref, local_sem.at[0])
    info_in = pltpu.make_async_copy(info_hbm, info_ref, local_sem.at[1])
    rows_in.start()
    info_in.start()
    landed = (landed_a, landed_b)
    for s in range(GROUPS):
        for spare in range(CAP, 2 * CAP):
            for h in range(2):
                landed[h][s, spare] = jnp.zeros((HALF, DIM), jnp.bfloat16)
    rows_in.wait()
    info_in.wait()
    for n in range(CAP):
        for h in range(2):
            landed[h][me_g, n] = rows_ref[me_g * CAP + n, HALF * h : HALF * h + HALF]
    pl.semaphore_wait(barrier, greeted)

    def remote(src, dst, send, recv, g, m):
        return pltpu.make_async_remote_copy(
            src_ref=src, dst_ref=dst, send_sem=send, recv_sem=recv,
            device_id=(g, m), device_id_type=MESH,
        )

    def row_copy(h, k, src_g):
        peer = (me_g + k) % GROUPS
        return remote(
            rows_ref.at[pl.ds(peer * CAP, CAP), pl.ds(HALF * h, HALF)],
            landed[h].at[src_g, pl.ds(0, CAP)],
            r_send.at[h, k], r_recv.at[h, src_g], peer, me_m,
        )

    def y_copy(h, k, j, slot):
        return remote(
            table.at[h, YS * k + j], y_parts.at[h, YS * k + slot],
            y_send.at[h, YS * k + j], y_recv.at[h, YS * k + slot], me_g, along(me_m, 0, j),
        )

    def z_copy(h, k, slot):
        return remote(
            z_sums.at[h, k], z_parts.at[h, slot], z_send.at[h, k], z_recv.at[h, slot],
            me_g, along(me_m, k, 0),
        )

    def total_of(h, owner):
        total = jnp.zeros((HALF, DIM), jnp.float32)
        for s in range(GROUPS):
            total += landed[h][s, info_ref[s, 0, INV_AT + owner] & (2 * CAP - 1)].astype(
                jnp.float32
            )
        return total

    mine = [None, None]

    def sum_y(h):
        for k in Z_FAR + (0,):
            total = total_of(h, along(me_m, k, 0))
            for j in (1, 3, 2):
                y_copy(h, k, j, j).wait_recv()
                total += y_parts[h, YS * k + j].astype(jnp.float32)
            if k:
                z_sums[h, k] = total.astype(jnp.bfloat16)
                z_copy(h, k, ZS - k).start()
            else:
                mine[h] = total

    for h in range(2):
        for k in (4, 5, 2, 3, 6, 7, 1):
            row_copy(h, k, me_g).start()
    for h in range(2):
        for k in range(1, GROUPS):
            row_copy(h, k, (me_g + k) % GROUPS).wait_recv()
        for k in Z_FAR + (0,):
            for j in Y_FAR:
                table[h, YS * k + j] = total_of(h, along(me_m, k, j)).astype(jnp.bfloat16)
                y_copy(h, k, j, YS - j).start()
    for h in range(2):
        sum_y(h)
    for h in range(2):
        for k in Z_NEAR:
            z_copy(h, k, k).wait_recv()
            mine[h] += z_parts[h, k].astype(jnp.float32)
        out_ref[0, HALF * h : HALF * h + HALF] = mine[h]
    for h in range(2):
        for k in range(1, GROUPS):
            row_copy(h, k, me_g).wait_send()
        for k in range(ZS):
            for j in range(1, YS):
                y_copy(h, k, j, j).wait_send()
            if k:
                z_copy(h, k, k).wait_send()


def give(rows, info):
    return pl.pallas_call(
        give_kernel,
        out_shape=jax.ShapeDtypeStruct((1, TOK, DIM), jnp.float32),
        in_specs=[
            pl.BlockSpec(memory_space=pl.ANY),
            pl.BlockSpec(memory_space=pl.ANY),
        ],
        out_specs=pl.BlockSpec(memory_space=pltpu.VMEM),
        scratch_shapes=[
            pltpu.VMEM((GROUPS * CAP, TOK, DIM), jnp.bfloat16),
            pltpu.SMEM(info.shape, jnp.int32),
            pltpu.VMEM((GROUPS, 2 * CAP, HALF, DIM), jnp.bfloat16),
            pltpu.VMEM((GROUPS, 2 * CAP, HALF, DIM), jnp.bfloat16),
            pltpu.VMEM((2, MEMBERS, HALF, DIM), jnp.bfloat16),
            pltpu.VMEM((2, MEMBERS, HALF, DIM), jnp.bfloat16),
            pltpu.VMEM((2, ZS, HALF, DIM), jnp.bfloat16),
            pltpu.VMEM((2, ZS, HALF, DIM), jnp.bfloat16),
            pltpu.SemaphoreType.DMA((2, GROUPS)),
            pltpu.SemaphoreType.DMA((2, GROUPS)),
            pltpu.SemaphoreType.DMA((2, MEMBERS)),
            pltpu.SemaphoreType.DMA((2, MEMBERS)),
            pltpu.SemaphoreType.DMA((2, ZS)),
            pltpu.SemaphoreType.DMA((2, ZS)),
            pltpu.SemaphoreType.DMA((2,)),
        ],
        compiler_params=pltpu.CompilerParams(
            collective_id=1, has_side_effects=True, vmem_limit_bytes=60 * 1024 * 1024
        ),
        name="give",
    )(rows, info)


def body(queries, pages, users, page_count, teacher):
    picked, place, info, page_t = fetch(queries, users, pages)
    scores, rows, page_grad = match(place, page_count, teacher, picked, pages, page_t)
    query_grad = give(rows, info)
    return scores, query_grad, page_grad


def solution(mesh):
    both = ("group", "member")
    three, two, one = P(both, None, None), P(both, None), P(both)
    return jax.shard_map(
        body,
        mesh=mesh,
        in_specs=(three, three, two, one, two),
        out_specs=(two, three, three),
        check_vma=False,
    )
```

```python
import functools
import math

import jax
import jax.numpy as jnp
from jax import lax
from jax.experimental import pallas as pl
from jax.experimental.pallas import tpu as pltpu
from jax.sharding import PartitionSpec as P

MESH = pl.DeviceIdType.MESH
CAP = 8
GROUPS = 8
MEMBERS = 32
TOK = 32
HALF = TOK // 2
ZS, YS = 8, 4
Z_FAR = (4, 3, 5, 2, 6, 1, 7)
Z_NEAR = (1, 7, 2, 6, 3, 5, 4)
Y_FAR = (2, 1, 3)
DIM = 128
CHUNK = 8
LANES = CHUNK * TOK
INV_AT = 32
SCALE = math.log2(math.e) / 0.05
LN2 = math.log(2.0)
TOP, PEAK, MASS, MOMENT, BASE, SLANT = range(6)


def along(me_m, dz, dy):
    return ((me_m // YS + dz) % ZS) * YS + (me_m % YS + dy) % YS


def greet(me_g, me_m):
    barrier = pltpu.get_barrier_semaphore()
    peers = [(me_g, along(me_m, k, 0)) for k in Z_FAR]
    peers += [(me_g, along(me_m, 0, k)) for k in range(1, YS)]
    peers += [((me_g + k) % GROUPS, me_m) for k in range(1, GROUPS)]
    for peer in peers:
        pl.semaphore_signal(barrier, inc=1, device_id=peer, device_id_type=MESH)
    return barrier, len(peers)


def fetch_kernel(
    query_hbm, users_hbm, pages_hbm, picked_hbm, place_hbm, info_hbm, page_t_hbm,
    table_a, table_b, users_ref, place_ref, pages_ref, page_t, asks_out, asks_in, asks_smem,
    chosen,
    z_send, y_send, q_recv, a_send, a_recv, c_send, c_recv, local_sem, in_sem, out_sem,
):
    me_g = lax.axis_index("group")
    me_m = lax.axis_index("member")
    n_pages = pages_hbm.shape[0]
    barrier, greeted = greet(me_g, me_m)
    users_in = pltpu.make_async_copy(users_hbm, users_ref, local_sem.at[0])
    table = (table_a, table_b)
    queries_in = [
        pltpu.make_async_copy(
            query_hbm.at[0, pl.ds(HALF * h, HALF)], table[h].at[me_m], local_sem.at[1 + 3 * h]
        )
        for h in range(2)
    ]
    users_in.start()
    for query_in in queries_in:
        query_in.start()

    def page_in(p):
        return pltpu.make_async_copy(pages_hbm.at[p], pages_ref.at[p], in_sem.at[p])

    def page_out(p):
        return pltpu.make_async_copy(page_t.at[p], page_t_hbm.at[p], out_sem.at[p])

    for p in range(n_pages):
        page_in(p).start()
    users_in.wait()

    total = GROUPS * MEMBERS
    rows = users_ref.shape[0]
    qid = lax.broadcasted_iota(jnp.int32, (total, users_ref.shape[1]), 0)
    hits = [jnp.where(users_ref[p : p + 1, :] == qid, 1.0, 0.0) for p in range(rows)]
    hit = functools.reduce(jnp.maximum, hits)
    count = lax.dot_general(
        jnp.ones((8, users_ref.shape[1]), jnp.bfloat16),
        hit.astype(jnp.bfloat16),
        (((1,), (1,)), ((), ())),
        preferred_element_type=jnp.float32,
    )
    used = jnp.where(count > 0.5, 1.0, 0.0)
    ri = lax.broadcasted_iota(jnp.int32, (total, total), 0)
    ci = lax.broadcasted_iota(jnp.int32, (total, total), 1)
    before = jnp.where((ri < ci) & ((ri >> 5) == (ci >> 5)), 1.0, 0.0).astype(jnp.bfloat16)
    rank = jnp.dot(used.astype(jnp.bfloat16), before, preferred_element_type=jnp.float32)
    lane8 = lax.broadcasted_iota(jnp.int32, (8, total), 1)
    sub8 = lax.broadcasted_iota(jnp.int32, (8, total), 0)
    of_group = (lane8 >> 5) == sub8
    k_id = lax.broadcasted_iota(jnp.int32, (128, total), 0).astype(jnp.float32)
    local_id = (lax.broadcasted_iota(jnp.int32, (128, total), 1) & 31).astype(jnp.float32)
    named = jnp.where((k_id == rank[0:1]) & (used[0:1] > 0.5), local_id, 0.0)
    ids = lax.dot_general(
        jnp.where(of_group, 1.0, 0.0).astype(jnp.bfloat16),
        named.astype(jnp.bfloat16),
        (((1,), (1,)), ((), ())),
        preferred_element_type=jnp.float32,
    )
    inverse = jnp.where(of_group, jnp.where(used > 0.5, rank, float(CAP)), 0.0)
    fold_r = lax.broadcasted_iota(jnp.int32, (total, 128), 0)
    fold_c = lax.broadcasted_iota(jnp.int32, (total, 128), 1)
    fold = jnp.where(fold_c == INV_AT + (fold_r & 31), 1.0, 0.0).astype(jnp.bfloat16)
    spread = jnp.dot(inverse.astype(jnp.bfloat16), fold, preferred_element_type=jnp.float32)
    asks = (ids + spread).astype(jnp.int32)
    for g in range(GROUPS):
        asks_out[g] = asks[g : g + 1, :]
    for query_in in queries_in:
        query_in.wait()

    def remote(src, dst, send, recv, g, m):
        return pltpu.make_async_remote_copy(
            src_ref=src, dst_ref=dst, send_sem=send, recv_sem=recv,
            device_id=(g, m), device_id_type=MESH,
        )

    def z_copy(h, k, src_m):
        return remote(
            table[h].at[src_m], table[h].at[src_m], z_send.at[h, k], q_recv.at[h, src_m],
            me_g, along(me_m, k, 0),
        )

    def y_copy(h, k, j, src_m):
        return remote(
            table[h].at[src_m], table[h].at[src_m],
            y_send.at[h, YS * k + j], q_recv.at[h, src_m], me_g, along(me_m, 0, j),
        )

    def ask_copy(k, src_g):
        peer = (me_g + k) % GROUPS
        return remote(
            asks_out.at[peer], asks_in.at[src_g], a_send.at[k], a_recv.at[src_g], peer, me_m
        )

    def chosen_copy(h, k, src_g):
        peer = (me_g + k) % GROUPS
        return remote(
            chosen.at[h, k], picked_hbm.at[pl.ds(src_g * CAP, CAP), pl.ds(HALF * h, HALF)],
            c_send.at[h, k], c_recv.at[h, src_g], peer, me_m,
        )

    pl.semaphore_wait(barrier, greeted)
    for k in range(1, GROUPS):
        ask_copy(k, me_g).start()
    for h in range(2):
        for k in Z_FAR:
            z_copy(h, k, me_m).start()
        for j in Y_FAR:
            y_copy(h, 0, j, me_m).start()
    asks_in[me_g] = asks_out[me_g]
    spot = ((lane8 >> 5) * CAP).astype(jnp.float32) + rank
    for p in range(rows):
        place = jnp.dot(
            spot.astype(jnp.bfloat16), hits[p].astype(jnp.bfloat16),
            preferred_element_type=jnp.float32,
        )
        place_ref[p : p + 1, :] = place[0:1].astype(jnp.int32)
    place_out = pltpu.make_async_copy(place_ref, place_hbm, local_sem.at[2])
    place_out.start()
    for p in range(n_pages):
        page_in(p).wait()
        page_t[p] = pages_ref[p].T
        page_out(p).start()
    for h in range(2):
        for k in Z_NEAR:
            src = along(me_m, k, 0)
            z_copy(h, k, src).wait_recv()
            for j in Y_FAR:
                y_copy(h, k, j, src).start()
    for k in range(1, GROUPS):
        ask_copy(k, (me_g + k) % GROUPS).wait_recv()
    to_smem = pltpu.make_async_copy(asks_in, asks_smem, local_sem.at[0])
    to_smem.start()
    info_out = pltpu.make_async_copy(asks_in, info_hbm, local_sem.at[3])
    info_out.start()
    to_smem.wait()
    owns = []
    for h in range(2):
        for k in (0,) + Z_NEAR:
            for j in range(1, YS):
                y_copy(h, k, j, along(me_m, k, j)).wait_recv()
        for k in (4, 5, 2, 3, 6, 7, 1, 0):
            peer = (me_g + k) % GROUPS
            for n in range(CAP):
                chosen[h, k, n] = table[h][asks_smem[peer, 0, n] & (MEMBERS - 1)]
            if k:
                chosen_copy(h, k, me_g).start()
        own = pltpu.make_async_copy(
            chosen.at[h, 0],
            picked_hbm.at[pl.ds(me_g * CAP, CAP), pl.ds(HALF * h, HALF)],
            local_sem.at[1 + 3 * h],
        )
        own.start()
        owns.append(own)
    for p in range(n_pages):
        page_out(p).wait()
    for h in range(2):
        for k in Z_NEAR:
            z_copy(h, k, me_m).wait_send()
        for k in (0,) + Z_NEAR:
            for j in range(1, YS):
                y_copy(h, k, j, along(me_m, k, 0)).wait_send()
        owns[h].wait()
    place_out.wait()
    info_out.wait()
    for k in range(1, GROUPS):
        ask_copy(k, me_g).wait_send()
        for h in range(2):
            chosen_copy(h, k, (me_g + k) % GROUPS).wait_recv()
            chosen_copy(h, k, me_g).wait_send()


def fetch(queries, users, pages):
    n_pages, n_tok, _ = pages.shape
    anywhere = pl.BlockSpec(memory_space=pl.ANY)
    return pl.pallas_call(
        fetch_kernel,
        out_shape=(
            jax.ShapeDtypeStruct((GROUPS * CAP, TOK, DIM), jnp.bfloat16),
            jax.ShapeDtypeStruct(users.shape, jnp.int32),
            jax.ShapeDtypeStruct((GROUPS, 1, 128), jnp.int32),
            jax.ShapeDtypeStruct((n_pages, DIM, n_tok), jnp.bfloat16),
        ),
        in_specs=[anywhere] * 3,
        out_specs=[anywhere] * 4,
        scratch_shapes=[
            pltpu.VMEM((MEMBERS, HALF, DIM), jnp.bfloat16),
            pltpu.VMEM((MEMBERS, HALF, DIM), jnp.bfloat16),
            pltpu.VMEM(users.shape, jnp.int32),
            pltpu.VMEM(users.shape, jnp.int32),
            pltpu.VMEM(pages.shape, jnp.bfloat16),
            pltpu.VMEM((n_pages, DIM, n_tok), jnp.bfloat16),
            pltpu.VMEM((GROUPS, 1, 128), jnp.int32),
            pltpu.VMEM((GROUPS, 1, 128), jnp.int32),
            pltpu.SMEM((GROUPS, 1, 128), jnp.int32),
            pltpu.VMEM((2, GROUPS, CAP, HALF, DIM), jnp.bfloat16),
            pltpu.SemaphoreType.DMA((2, ZS)),
            pltpu.SemaphoreType.DMA((2, MEMBERS)),
            pltpu.SemaphoreType.DMA((2, MEMBERS)),
            pltpu.SemaphoreType.DMA((GROUPS,)),
            pltpu.SemaphoreType.DMA((GROUPS,)),
            pltpu.SemaphoreType.DMA((2, GROUPS)),
            pltpu.SemaphoreType.DMA((2, GROUPS)),
            pltpu.SemaphoreType.DMA((5,)),
            pltpu.SemaphoreType.DMA((n_pages,)),
            pltpu.SemaphoreType.DMA((n_pages,)),
        ],
        compiler_params=pltpu.CompilerParams(
            collective_id=0, has_side_effects=True, vmem_limit_bytes=60 * 1024 * 1024
        ),
        name="fetch",
    )(queries, users, pages)


def split_dot(value, ones):
    high = value.astype(jnp.bfloat16)
    rest = value - high.astype(jnp.float32)
    mid = rest.astype(jnp.bfloat16)
    low = (rest - mid.astype(jnp.float32)).astype(jnp.bfloat16)
    dot = functools.partial(jnp.dot, preferred_element_type=jnp.float32)
    return dot(high, ones) + (dot(mid, ones) + dot(low, ones))


def match_kernel(
    place_hbm, count_hbm, teacher_hbm, picked_hbm, pages_hbm, page_t_hbm,
    scores_hbm, rows_hbm, grad_hbm,
    chunks, place_ref, count_ref, teacher_ref, picked_ref, scaled, pages_ref, page_t, sims, logit, pending, stats, acc,
    grad_ref, row_acc, score_l, same_slot, scores_ref, rows_ref, in_sem, out_sem, small_sem,
):
    n_pages, n_tok, _ = pages_ref.shape
    per_page = place_ref.shape[1] // CHUNK
    half = n_tok // 2
    quarter = n_tok // 4

    def page_in(p):
        return pltpu.make_async_copy(pages_hbm.at[p], pages_ref.at[p], in_sem.at[p])

    picked_in = pltpu.make_async_copy(picked_hbm, picked_ref, in_sem.at[n_pages])
    turned_in = pltpu.make_async_copy(page_t_hbm, page_t, in_sem.at[n_pages + 1])
    smalls = [
        pltpu.make_async_copy(source, dest, small_sem.at[i])
        for i, (source, dest) in enumerate(
            ((count_hbm, count_ref), (place_hbm, place_ref), (teacher_hbm, teacher_ref))
        )
    ]
    for small in smalls:
        small.start()
    picked_in.start()
    for p in range(n_pages):
        page_in(p).start()
    turned_in.start()

    acc[...] = jnp.zeros_like(acc)
    row_acc[...] = jnp.zeros_like(row_acc)
    score_l[...] = jnp.zeros_like(score_l)
    logit[...] = jnp.zeros_like(logit)
    stats[...] = jnp.zeros_like(stats)
    pending[...] = jnp.zeros_like(pending)
    seg_r = lax.broadcasted_iota(jnp.int32, (LANES, LANES), 0) >> 5
    seg_c = lax.broadcasted_iota(jnp.int32, (LANES, LANES), 1) >> 5
    same_slot[...] = jnp.where(seg_r == seg_c, 1.0, 0.0).astype(jnp.bfloat16)
    slot_of_lane = lax.broadcasted_iota(jnp.int32, (8, LANES), 1) >> 5
    for small in smalls:
        small.wait()

    def list_chunk(n, total):
        p = n // per_page
        alive = (n % per_page) * CHUNK < count_ref[p]

        @pl.when(alive)
        def _():
            chunks[total] = n

        return total + alive.astype(jnp.int32)

    total = lax.fori_loop(0, n_pages * per_page, list_chunk, jnp.int32(0))
    for n in range(3):
        chunks[total + n] = 0
    pairs = (total + 1) // 2
    picked_in.wait()

    def scale_picked(n, carry):
        full = picked_ref[n].astype(jnp.float32) * SCALE
        high = full.astype(jnp.bfloat16)
        scaled[n, :, :DIM] = high
        scaled[n, :, DIM:] = (full - high.astype(jnp.float32)).astype(jnp.bfloat16)
        return carry

    lax.fori_loop(0, picked_ref.shape[0], scale_picked, 0, unroll=8)
    for p in range(2):
        page_in(p).wait()

    def where_of(n):
        code = chunks[n]
        return code // per_page, code % per_page

    def chosen_of(p, c, source):
        return jnp.concatenate(
            [source[place_ref[p, c * CHUNK + k]] for k in range(CHUNK)], axis=0
        )

    def fold8(value, op):
        parts = [value[8 * i : 8 * i + 8] for i in range(value.shape[0] // 8)]
        while len(parts) > 1:
            parts = [
                op(parts[i], parts[i + 1]) if i + 1 < len(parts) else parts[i]
                for i in range(0, len(parts), 2)
            ]
        return parts[0]

    def tall(value, rows):
        return jnp.concatenate([value] * (rows // 8), axis=0)

    def similar_half(p, chosen, slot, h):
        at = slice(half * h, half * h + half)
        page = pages_ref[p, at, :]
        block = lax.dot_general(
            jnp.concatenate([page, page], axis=1), chosen, (((1,), (1,)), ((), ())),
            preferred_element_type=jnp.float32,
        )
        sims[slot, at, :] = block
        return fold8(block, jnp.maximum)

    def similar(n, slot):
        p, c = where_of(n)
        chosen = chosen_of(p, c, scaled)
        tops = [similar_half(p, chosen, slot, h) for h in range(2)]
        stats[slot, TOP] = jnp.maximum(*tops)

    def weigh_rows(slot, top, start, rows):
        mass = moment = None
        for i in range(rows // 32):
            at = slice(start + 32 * i, start + 32 * i + 32)
            t = sims[slot, at, :] - tall(top, 32)
            e = jnp.exp2(t)
            g = e * t
            logit[slot, at, :] = t
            e, g = fold8(e, jnp.add), fold8(g, jnp.add)
            mass = e if mass is None else mass + e
            moment = g if moment is None else moment + g
        return mass, moment

    def settle(n, slot, begun):
        p, c = where_of(n)
        known = (n < total) & begun
        mass = jnp.broadcast_to(
            jnp.sum(stats[slot, MASS], axis=0, keepdims=True), (8, LANES)
        )
        moment = jnp.broadcast_to(
            jnp.sum(stats[slot, MOMENT], axis=0, keepdims=True), (8, LANES)
        )
        mass = jnp.where(mass > 0.0, mass, 1.0)
        mean = moment / mass
        matched = (stats[slot, PEAK] + mean) * (1.0 / SCALE)
        score = split_dot(matched, same_slot[...])
        taught = jnp.zeros((8, LANES), jnp.float32)
        for k in range(CHUNK):
            taught = jnp.where(slot_of_lane == k, teacher_ref[p, c * CHUNK + k], taught)
        bound = jnp.where(known, count_ref[p] - c * CHUNK, 0)
        live = slot_of_lane < bound
        row = jnp.where(known, p, n_pages)
        score_l[c, pl.ds(row, 1), :] = jnp.where(live, score, 0.0)[0:1]
        part = jnp.where(live, (score - taught) / mass, 0.0)
        slant = part * LN2
        stats[slot, BASE] = part - slant * mean
        stats[slot, SLANT] = slant

    def slope_rows(slot, base, slant, start, rows):
        parts = []
        for i in range(rows // 32):
            at = slice(start + 32 * i, start + 32 * i + 32)
            t = logit[slot, at, :]
            parts.append(
                (jnp.exp2(t) * (tall(base, 32) + tall(slant, 32) * t)).astype(jnp.bfloat16)
            )
        return jnp.concatenate(parts, axis=0)

    def spread_rows(p, chosen, slope, at, query_t):
        acc[p, at, :] += jnp.dot(slope, chosen, preferred_element_type=jnp.float32)
        part = jnp.dot(page_t[p, :, at], slope, preferred_element_type=jnp.float32)
        return part if query_t is None else query_t + part

    def add_rows(n, slot):
        p, c = where_of(n)
        query_part = pending[slot].T
        for k in range(CHUNK):
            row_acc[place_ref[p, c * CHUNK + k]] += query_part[TOK * k : TOK * k + TOK]

    def spread(n, slot):
        p, c = where_of(n)
        chosen = chosen_of(p, c, picked_ref)
        base, slant = stats[slot, BASE], stats[slot, SLANT]
        query_t = None
        for b in range(4):
            at = slice(quarter * b, quarter * b + quarter)
            slope = slope_rows(slot, base, slant, quarter * b, quarter)
            query_t = spread_rows(p, chosen, slope, at, query_t)
        pending[slot] = query_t

    def turn(old, now, new, slot):
        p_old, c_old = where_of(old)
        p_new, c_new = where_of(new)
        chosen_old = chosen_of(p_old, c_old, picked_ref)
        chosen_new = chosen_of(p_new, c_new, scaled)
        base, slant = stats[slot, BASE], stats[slot, SLANT]
        top = jnp.broadcast_to(
            jnp.max(stats[slot, TOP], axis=0, keepdims=True), (8, LANES)
        )
        stats[slot, PEAK] = top
        query_t = mass = moment = None
        tops = []
        for h in range(2):
            for b in (2 * h, 2 * h + 1):
                at = slice(quarter * b, quarter * b + quarter)
                slope = slope_rows(slot, base, slant, quarter * b, quarter)
                query_t = spread_rows(p_old, chosen_old, slope, at, query_t)
                e, g = weigh_rows(slot, top, quarter * b, quarter)
                mass = e if mass is None else mass + e
                moment = g if moment is None else moment + g
            tops.append(similar_half(p_new, chosen_new, slot, h))
        stats[slot, TOP] = jnp.maximum(*tops)
        stats[slot, MASS] = mass
        stats[slot, MOMENT] = moment
        pending[slot] = query_t

    similar(0, 0)
    similar(1, 1)
    for p in range(2, n_pages):
        page_in(p).wait()
    turned_in.wait()

    def step(i, carry):
        n = 2 * i
        old = jnp.maximum(n - 2, 0)

        settle(old + 1, 1, i > 0)
        add_rows(jnp.maximum(n - 3, 0), 1)
        turn(old, n, n + 2, 0)
        settle(n, 0, True)
        add_rows(old, 0)
        turn(old + 1, n + 1, n + 3, 1)
        return carry

    lax.fori_loop(0, pairs, step, 0)

    def page_out(p):
        return pltpu.make_async_copy(grad_ref.at[p], grad_hbm.at[p], out_sem.at[p])

    for p in range(n_pages - 2):
        grad_ref[p] = acc[p].astype(jnp.bfloat16)
        page_out(p).start()
    last = 2 * pairs - 1
    settle(last, 1, True)
    add_rows(jnp.maximum(last - 2, 0), 1)
    spread(last - 1, 0)
    spread(last, 1)
    for p in range(n_pages - 2, n_pages):
        grad_ref[p] = acc[p].astype(jnp.bfloat16)
        page_out(p).start()
    add_rows(last - 1, 0)
    add_rows(last, 1)
    rows_ref[...] = row_acc[...].astype(jnp.bfloat16)
    rows_out = pltpu.make_async_copy(rows_ref, rows_hbm, small_sem.at[0])
    rows_out.start()
    col = lax.broadcasted_iota(jnp.int32, (LANES, 128), 1)
    row = lax.broadcasted_iota(jnp.int32, (LANES, 128), 0)
    out = jnp.zeros((8, 128), jnp.float32)
    for c in range(per_page):
        take = jnp.where(row == (col - c * CHUNK) * TOK, 1.0, 0.0)
        out += split_dot(score_l[c], take.astype(jnp.bfloat16))
    scores_ref[...] = out[: scores_ref.shape[0], : scores_ref.shape[1]]
    scores_out = pltpu.make_async_copy(scores_ref, scores_hbm, small_sem.at[1])
    scores_out.start()
    rows_out.wait()
    scores_out.wait()
    for p in range(n_pages):
        page_out(p).wait()


def match(place, page_count, teacher, picked, pages, page_t):
    n_pages, n_tok, _ = pages.shape
    per_page = teacher.shape[1] // CHUNK
    anywhere = pl.BlockSpec(memory_space=pl.ANY)
    return pl.pallas_call(
        match_kernel,
        out_shape=(
            jax.ShapeDtypeStruct(teacher.shape, jnp.float32),
            jax.ShapeDtypeStruct(picked.shape, jnp.bfloat16),
            jax.ShapeDtypeStruct(pages.shape, jnp.bfloat16),
        ),
        in_specs=[anywhere] * 6,
        out_specs=[anywhere] * 3,
        scratch_shapes=[
            pltpu.SMEM((n_pages * per_page + 3,), jnp.int32),
            pltpu.SMEM(place.shape, jnp.int32),
            pltpu.SMEM(page_count.shape, jnp.int32),
            pltpu.SMEM(teacher.shape, jnp.float32),
            pltpu.VMEM(picked.shape, jnp.bfloat16),
            pltpu.VMEM((GROUPS * CAP, TOK, 2 * DIM), jnp.bfloat16),
            pltpu.VMEM(pages.shape, jnp.bfloat16),
            pltpu.VMEM((n_pages, DIM, n_tok), jnp.bfloat16),
            pltpu.VMEM((2, n_tok, LANES), jnp.float32),
            pltpu.VMEM((2, n_tok, LANES), jnp.float32),
            pltpu.VMEM((2, DIM, LANES), jnp.float32),
            pltpu.VMEM((2, 6, 8, LANES), jnp.float32),
            pltpu.VMEM((n_pages, n_tok, DIM), jnp.float32),
            pltpu.VMEM(pages.shape, jnp.bfloat16),
            pltpu.VMEM(picked.shape, jnp.float32),
            pltpu.VMEM((per_page, 8, LANES), jnp.float32),
            pltpu.VMEM((LANES, LANES), jnp.bfloat16),
            pltpu.VMEM(teacher.shape, jnp.float32),
            pltpu.VMEM(picked.shape, jnp.bfloat16),
            pltpu.SemaphoreType.DMA((n_pages + 2,)),
            pltpu.SemaphoreType.DMA((n_pages,)),
            pltpu.SemaphoreType.DMA((3,)),
        ],
        compiler_params=pltpu.CompilerParams(vmem_limit_bytes=60 * 1024 * 1024),
        name="match",
    )(place, page_count, teacher, picked, pages, page_t)


def give_kernel(
    rows_hbm, info_hbm, out_ref,
    rows_ref, info_ref, landed_a, landed_b, table, y_parts, z_sums, z_parts,
    r_send, r_recv, y_send, y_recv, z_send, z_recv, local_sem,
):
    me_g = lax.axis_index("group")
    me_m = lax.axis_index("member")
    barrier, greeted = greet(me_g, me_m)
    rows_in = pltpu.make_async_copy(rows_hbm, rows_ref, local_sem.at[0])
    info_in = pltpu.make_async_copy(info_hbm, info_ref, local_sem.at[1])
    rows_in.start()
    info_in.start()
    landed = (landed_a, landed_b)
    for s in range(GROUPS):
        for spare in range(CAP, 2 * CAP):
            for h in range(2):
                landed[h][s, spare] = jnp.zeros((HALF, DIM), jnp.bfloat16)
    rows_in.wait()
    info_in.wait()
    for n in range(CAP):
        for h in range(2):
            landed[h][me_g, n] = rows_ref[me_g * CAP + n, HALF * h : HALF * h + HALF]
    pl.semaphore_wait(barrier, greeted)

    def remote(src, dst, send, recv, g, m):
        return pltpu.make_async_remote_copy(
            src_ref=src, dst_ref=dst, send_sem=send, recv_sem=recv,
            device_id=(g, m), device_id_type=MESH,
        )

    def row_copy(h, k, src_g):
        peer = (me_g + k) % GROUPS
        return remote(
            rows_ref.at[pl.ds(peer * CAP, CAP), pl.ds(HALF * h, HALF)],
            landed[h].at[src_g, pl.ds(0, CAP)],
            r_send.at[h, k], r_recv.at[h, src_g], peer, me_m,
        )

    def y_copy(h, k, j, slot):
        return remote(
            table.at[h, YS * k + j], y_parts.at[h, YS * k + slot],
            y_send.at[h, YS * k + j], y_recv.at[h, YS * k + slot], me_g, along(me_m, 0, j),
        )

    def z_copy(h, k, slot):
        return remote(
            z_sums.at[h, k], z_parts.at[h, slot], z_send.at[h, k], z_recv.at[h, slot],
            me_g, along(me_m, k, 0),
        )

    def total_of(h, owner):
        total = jnp.zeros((HALF, DIM), jnp.float32)
        for s in range(GROUPS):
            total += landed[h][s, info_ref[s, 0, INV_AT + owner] & (2 * CAP - 1)].astype(
                jnp.float32
            )
        return total

    mine = [None, None]

    def sum_y(h):
        for k in Z_FAR + (0,):
            total = total_of(h, along(me_m, k, 0))
            for j in (1, 3, 2):
                y_copy(h, k, j, j).wait_recv()
                total += y_parts[h, YS * k + j].astype(jnp.float32)
            if k:
                z_sums[h, k] = total.astype(jnp.bfloat16)
                z_copy(h, k, ZS - k).start()
            else:
                mine[h] = total

    for h in range(2):
        for k in (4, 5, 2, 3, 6, 7, 1):
            row_copy(h, k, me_g).start()
    for h in range(2):
        for k in range(1, GROUPS):
            row_copy(h, k, (me_g + k) % GROUPS).wait_recv()
        for k in Z_FAR + (0,):
            for j in Y_FAR:
                table[h, YS * k + j] = total_of(h, along(me_m, k, j)).astype(jnp.bfloat16)
                y_copy(h, k, j, YS - j).start()
    for h in range(2):
        sum_y(h)
    for h in range(2):
        for k in Z_NEAR:
            z_copy(h, k, k).wait_recv()
            mine[h] += z_parts[h, k].astype(jnp.float32)
        out_ref[0, HALF * h : HALF * h + HALF] = mine[h]
    for h in range(2):
        for k in range(1, GROUPS):
            row_copy(h, k, me_g).wait_send()
        for k in range(ZS):
            for j in range(1, YS):
                y_copy(h, k, j, j).wait_send()
            if k:
                z_copy(h, k, k).wait_send()


def give(rows, info):
    return pl.pallas_call(
        give_kernel,
        out_shape=jax.ShapeDtypeStruct((1, TOK, DIM), jnp.float32),
        in_specs=[
            pl.BlockSpec(memory_space=pl.ANY),
            pl.BlockSpec(memory_space=pl.ANY),
        ],
        out_specs=pl.BlockSpec(memory_space=pltpu.VMEM),
        scratch_shapes=[
            pltpu.VMEM((GROUPS * CAP, TOK, DIM), jnp.bfloat16),
            pltpu.SMEM(info.shape, jnp.int32),
            pltpu.VMEM((GROUPS, 2 * CAP, HALF, DIM), jnp.bfloat16),
            pltpu.VMEM((GROUPS, 2 * CAP, HALF, DIM), jnp.bfloat16),
            pltpu.VMEM((2, MEMBERS, HALF, DIM), jnp.bfloat16),
            pltpu.VMEM((2, MEMBERS, HALF, DIM), jnp.bfloat16),
            pltpu.VMEM((2, ZS, HALF, DIM), jnp.bfloat16),
            pltpu.VMEM((2, ZS, HALF, DIM), jnp.bfloat16),
            pltpu.SemaphoreType.DMA((2, GROUPS)),
            pltpu.SemaphoreType.DMA((2, GROUPS)),
            pltpu.SemaphoreType.DMA((2, MEMBERS)),
            pltpu.SemaphoreType.DMA((2, MEMBERS)),
            pltpu.SemaphoreType.DMA((2, ZS)),
            pltpu.SemaphoreType.DMA((2, ZS)),
            pltpu.SemaphoreType.DMA((2,)),
        ],
        compiler_params=pltpu.CompilerParams(
            collective_id=1, has_side_effects=True, vmem_limit_bytes=60 * 1024 * 1024
        ),
        name="give",
    )(rows, info)


def body(queries, pages, users, page_count, teacher):
    picked, place, info, page_t = fetch(queries, users, pages)
    scores, rows, page_grad = match(place, page_count, teacher, picked, pages, page_t)
    query_grad = give(rows, info)
    return scores, query_grad, page_grad


def solution(mesh):
    both = ("group", "member")
    three, two, one = P(both, None, None), P(both, None), P(both)
    return jax.shard_map(
        body,
        mesh=mesh,
        in_specs=(three, three, two, one, two),
        out_specs=(two, three, three),
        check_vma=False,
    )
```
